32 devices in a mesh: groups: 2 (over x), owner: 16 (over z, y, core).
Axes of the slice: x: 2, y: 2, z: 4, core: 2. Of those that a mesh axis runs over, the one named last changes fastest.
Arguments:
- queries: bfloat16 [2048, 1024], P(('groups', 'owner')), parts along dimension 0, may hold values from -0.3984375 to 0.3984375
- probes: int32 [2048, 8], P(('groups', 'owner')), parts along dimension 0, may hold values from 0 to 255, as said below
- passages: bfloat16 [256, 256, 1024], P('owner'), may hold values from -6 to 6
- centroids: bfloat16 [256, 1024], P('owner'), may hold values from -6 to 6
- counts: int32 [256], P('owner'), may hold values from 1 to 256
Outputs:
- scores: float32 [2048, 8, 256], P(('groups', 'owner')), parts along dimension 0
- visits: int32 [2048], P(('groups', 'owner')), parts along dimension 0
The draws below stay inside these ranges and needn't reach their ends.
There are 2 independent parts, one for each index of `groups`. The reference program is written for one: setup_inputs(seed, part) draws one part's arguments, and reference() takes and returns one part's arrays. A program takes and returns all parts, laid end to end along the dimension named above; an argument that names none is the same for every part. Nothing has to cross between parts.
Inputs may be any that keep to these rules, and one draw needn't show every extreme that they name: Cluster c belongs to owner index c // 16. In each aligned block of 64 queries (the queries of one index of owner) at most 64 probes name clusters of one owner, and in every draw some owners receive exactly 64 probes from every block. A query may name a cluster more than once.
All inputs are finite; a program needn't handle non-finite values.
Results may differ from the reference program's by a relative error of at most 0.0003.
Values may be sent and summed in bfloat16 or wider, within the bound.
A program may use at most 64 MiB of HBM per device.

```python
import jax
import jax.numpy as jnp
from jax import lax

D = 1024
PASSAGES = 256
PROBES = 8
Q_DEV = 64
CL_DEV = 16
QUERIES = 1024
CLUSTERS = 256
CAP = 64


def draw_probes(key, part):
    owner_total = CLUSTERS // CL_DEV
    slot_total = owner_total * CAP
    pick_total = Q_DEV * PROBES
    hot_key, rest_key = jax.random.split(jax.random.fold_in(key, 17))
    shuffled = jax.random.permutation(hot_key, owner_total)
    hotness = (shuffled < owner_total // 8).astype(jnp.int32)
    source_keys = jax.random.split(rest_key, owner_total)

    def one_source(source_key):
        key_prio, key_order, key_local = jax.random.split(source_key, 3)
        positions = jnp.arange(slot_total, dtype=jnp.int32)
        slot_owner = positions // CAP
        priority = jax.random.randint(key_prio, (slot_total,), 0, 1024) + hotness[slot_owner] * 2048
        priority = priority * slot_total + positions
        unused, chosen = lax.top_k(priority, pick_total)
        chosen = jax.random.permutation(key_order, chosen)
        local_ids = jax.random.randint(key_local, (pick_total,), 0, CL_DEV)
        return (chosen // CAP * CL_DEV + local_ids).astype(jnp.int32).reshape(Q_DEV, PROBES)
    return jax.vmap(one_source)(source_keys).reshape(QUERIES, PROBES)


def plant(values, stream_key, least, top_value):
    longest = values.shape.index(max(values.shape))
    spots = []
    for shift in (0, 1):
        where = [jax.random.randint(jax.random.fold_in(stream_key, axis), (), 0, length) for axis, length in enumerate(values.shape)]
        where[longest] = (where[longest] + shift) % values.shape[longest]
        spots.append(tuple(where))
    return values.at[spots[0]].set(least).at[spots[1]].set(top_value)


def steps_of(rng, extent, shards, smallest, high):
    factor_of, own = 1.0, jax.random.fold_in(rng, 6)
    for position, blocks in shards:
        steps = jnp.exp(jax.random.uniform(jax.random.fold_in(own, position), (blocks,), jnp.float32, smallest / len(shards), high / len(shards)))
        factor_of = factor_of * jnp.repeat(steps, extent[position] // blocks).reshape([-1 if axis == position else 1 for axis in range(len(extent))])
    return factor_of


def bell_draw(stream_key, dims, scale, reach, shards=(), kind=jnp.bfloat16):
    drawn = scale * jax.random.normal(stream_key, dims, jnp.float32)
    if shards:
        drawn = drawn * steps_of(stream_key, dims, shards, -0.22, 0.18)
    return jnp.clip(drawn, -reach, reach).astype(kind)


def setup_inputs(seed: int = 0, part: int = 0) -> dict:
    key_of = jax.random.split(jax.random.key(seed), 6)
    part_splits = jax.random.split(jax.random.fold_in(key_of[5], part), 6)
    return {
        "queries": bell_draw(part_splits[0], (QUERIES, D), 0.05, 0.3984375, ((0, 16),)),
        "probes": draw_probes(jax.random.fold_in(jax.random.fold_in(key_of[5], part), 71), part),
        "passages": bell_draw(key_of[2], (CLUSTERS, PASSAGES, D), 1.0, 6.0, ((0, 16),)),
        "centroids": bell_draw(key_of[3], (CLUSTERS, D), 1.0, 6.0, ((0, 16),)),
        "counts": plant(jax.random.randint(key_of[4], (CLUSTERS,), 1, PASSAGES + 1), jax.random.fold_in(key_of[4], 1), 1, PASSAGES).astype(jnp.int32),
    }


def reference(queries, probes, passages, centroids, counts):
    query_count, probe_count = probes.shape
    pair_count = query_count * probe_count
    block_size = 256
    cluster_list = probes.reshape(pair_count // block_size, block_size).astype(jnp.int32)
    query_list = (jnp.arange(pair_count, dtype=jnp.int32) // probe_count).reshape(pair_count // block_size, block_size)

    def score_block(pieces):
        cluster_ids, query_ids = pieces
        query_rows = queries[query_ids].astype(jnp.float32)
        chosen = passages[cluster_ids].astype(jnp.float32)
        direct = jnp.einsum('bd,btd->bt', query_rows, chosen)
        centre = jnp.sum(query_rows * centroids[cluster_ids].astype(jnp.float32), axis=1)
        live_mask = jnp.arange(PASSAGES, dtype=jnp.int32)[None, :] < counts[cluster_ids][:, None]
        return jnp.where(live_mask, direct + centre[:, None], jnp.float32(0.0))

    scores = lax.map(score_block, (cluster_list, query_list)).reshape(query_count, probe_count, PASSAGES)
    visits = jnp.sum(counts[probes], axis=1).astype(jnp.int32)
    return scores, visits
```

```python
import jax
import jax.numpy as jnp
from jax import lax
from jax.experimental import pallas as pl
from jax.experimental.pallas import tpu as pltpu
from jax.sharding import PartitionSpec as P


def routed_body(queries, probes, passages, centroids, counts):
    owner_count = lax.axis_size("owner")
    per_device, probe_count = probes.shape
    local_count, block_span, feature_width = passages.shape
    capacity = 2 * per_device * probe_count // owner_count
    pair_count = per_device * probe_count
    passage_blocks = jnp.transpose(passages, (0, 2, 1))
    flat_probes = probes.reshape(-1)
    target_owner = flat_probes // local_count
    target_local = flat_probes % local_count
    owner_hits = (
        target_owner[:, None] == jnp.arange(owner_count, dtype=jnp.int32)[None, :]
    ).astype(jnp.int32)
    slot_rank = jnp.sum((jnp.cumsum(owner_hits, axis=0) - owner_hits) * owner_hits, axis=1)
    slot_index = target_owner * capacity + slot_rank
    pair_ids = jnp.arange(pair_count, dtype=jnp.int32)
    slot_match = slot_index[None, :] == jnp.arange(owner_count * capacity, dtype=jnp.int32)[:, None]
    slot_filled = jnp.any(slot_match, axis=1)
    source_pair = jnp.sum(jnp.where(slot_match, pair_ids[None, :], 0), axis=1)
    send_rows = jnp.where(
        slot_filled[:, None], queries[source_pair // probe_count], jnp.zeros((), jnp.bfloat16)
    )
    send_ids = jnp.where(slot_filled, target_local[source_pair], -1)
    query_rows = lax.all_to_all(
        send_rows.reshape(owner_count, capacity, feature_width),
        "owner",
        split_axis=0,
        concat_axis=0,
        tiled=True,
    )
    cluster_ids = lax.all_to_all(
        send_ids.reshape(owner_count, capacity), "owner", split_axis=0, concat_axis=0, tiled=True
    )
    source_count, slot_count = cluster_ids.shape
    row_total = source_count * slot_count
    flat_rows = query_rows.reshape(row_total, feature_width)
    flat_ids = cluster_ids.reshape(-1)
    group_ids = jnp.where(flat_ids < 0, 0, flat_ids).astype(jnp.int32)
    cluster_pick = flat_ids[:, None] == jnp.arange(local_count, dtype=jnp.int32)[None, :]
    live_sizes = jnp.sum(jnp.where(cluster_pick, counts[None, :], 0), axis=1)
    group_pick = group_ids[:, None] == jnp.arange(local_count, dtype=jnp.int32)[None, :]
    group_sizes = jnp.sum(group_pick.astype(jnp.int32), axis=0)
    order = jnp.argsort(group_ids, stable=True)
    undo_order = jnp.argsort(order, stable=True)
    sorted_rows = flat_rows[order]
    sorted_scores = lax.ragged_dot(
        sorted_rows, passage_blocks, group_sizes, preferred_element_type=jnp.float32
    )
    own_scores = sorted_scores[undo_order]
    centre_term = jnp.einsum(
        "rd,rd->r", flat_rows, centroids[group_ids], preferred_element_type=jnp.float32
    )
    live_mask = jnp.arange(block_span, dtype=jnp.int32)[None, :] < live_sizes[:, None]
    masked_scores = jnp.where(live_mask, own_scores + centre_term[:, None], 0.0)
    back_scores = lax.all_to_all(
        masked_scores.reshape(source_count, slot_count, block_span),
        "owner",
        split_axis=0,
        concat_axis=0,
        tiled=True,
    )
    back_sizes = lax.all_to_all(
        live_sizes.astype(jnp.float32).reshape(source_count, slot_count),
        "owner",
        split_axis=0,
        concat_axis=0,
        tiled=True,
    )
    flat_scores = back_scores.reshape(owner_count * capacity, block_span)
    scores = flat_scores[slot_index].reshape(per_device, probe_count, block_span)
    pair_sizes = back_sizes.reshape(-1)[slot_index].reshape(per_device, probe_count)
    visits = jnp.sum(pair_sizes, axis=1).astype(jnp.int32)
    return (scores, visits)


LANES = 128
GROUP = 4
TOP = 32767.0


def owner_kernel(
    n, q_hbm, probe_hbm, pass_hbm, cent_hbm, cnt_hbm,
    out_ref, vis_ref,
    pass_v, qs, cent_v, cnt_v, probe_v, ms, slots, rows_v, acc, cntb, sendb, sends, recvb, recvs, cnt_s,
    pass_sem, load_sem, qsend, msend, qrecv, mrecv, bsend, ssend, brecv, srecv,
):
    clusters, width = cent_v.shape
    span = pass_v.shape[0] // clusters
    probe_count, per_device = probe_v.shape
    pairs = probe_count * per_device
    planes = n // 4
    rows = 4 * per_device
    tables = ms.shape[1] - 1
    cap = LANES // 2
    wide = 4 * cap
    half = span // 2
    piece = per_device // 2
    code_bits = (clusters * per_device).bit_length() - 1
    q_bits = per_device.bit_length() - 1
    cl_bits = clusters.bit_length() - 1
    me = lax.axis_index("owner")
    z = me // 4
    y = (me // 2) % 2
    c = me % 2
    y_dev = z * 4 + (1 - y) * 2 + c
    c_dev = z * 4 + y * 2 + (1 - c)
    has_low = z > 0
    has_high = z < planes - 1

    loads = [
        pltpu.make_async_copy(q_hbm, qs.at[me], load_sem.at[0]),
        pltpu.make_async_copy(probe_hbm, probe_v, load_sem.at[1]),
        pltpu.make_async_copy(cnt_hbm, cnt_v, load_sem.at[2]),
        pltpu.make_async_copy(cent_hbm, cent_v, load_sem.at[3]),
    ]
    for copy in loads:
        copy.start()

    barrier = pltpu.get_barrier_semaphore()

    def greet(dev):
        pl.semaphore_signal(barrier, inc=1, device_id={"owner": dev})

    greet(y_dev)
    greet(c_dev)

    @pl.when(has_low)
    def _():
        greet(me - 4)

    @pl.when(has_high)
    def _():
        greet(me + 4)

    def passage_copy(k):
        return pltpu.make_async_copy(pass_hbm.at[k], pass_v.at[pl.ds(k * span, span)], pass_sem.at[k])

    for k in range(clusters):
        passage_copy(k).start()

    loads[0].wait()
    pl.semaphore_wait(barrier, 2 + jnp.where(has_low, 1, 0) + jnp.where(has_high, 1, 0))

    def chunk(s, h, target, dev):
        if h == 2:
            return pltpu.make_async_remote_copy(
                src_ref=ms.at[s], dst_ref=ms.at[s],
                send_sem=msend.at[s, target], recv_sem=mrecv.at[s], device_id={"owner": dev},
            )
        cut = pl.ds(h * piece, piece)
        return pltpu.make_async_remote_copy(
            src_ref=qs.at[s, cut], dst_ref=qs.at[s, cut],
            send_sem=qsend.at[s, h, target], recv_sem=qrecv.at[s, h], device_id={"owner": dev},
        )

    def push(s, h, target, dev):
        chunk(s, h, target, dev).start()

    def drain(s, h, target, dev):
        chunk(s, h, target, dev).wait_send()

    def arrive(s, h):
        chunk(s, h, 0, c_dev).wait_recv()

    def onward(act, s, h, low, high):
        @pl.when(low)
        def _():
            act(s, h, 0, me - 4)

        @pl.when(high)
        def _():
            act(s, h, 1, me + 4)

        act(s, h, 2, y_dev)
        act(s, h, 3, c_dev)

    for h in range(2):
        onward(push, me, h, has_low, has_high)

    for copy in loads[1:]:
        copy.wait()

    def lower(row):
        return jnp.where(c == 1, pltpu.roll(row, cap, 1), row)

    def upper(row):
        return jnp.where(c == 1, row, pltpu.roll(row, cap, 1))

    lane_row = lax.broadcasted_iota(jnp.int32, (8, LANES), 1)

    def join(first, second):
        first = jnp.broadcast_to(first, (8, LANES))
        second = jnp.broadcast_to(second, (8, LANES))
        return jnp.where(lane_row < cap, lower(first), upper(second))[0:1]

    probes = probe_v[...]
    target = probes >> cl_bits
    local = probes & (clusters - 1)
    hits = jnp.concatenate(
        [jnp.where(target == o, 1.0, 0.0).astype(jnp.float32) for o in range(n)], axis=0
    ).astype(jnp.bfloat16)
    big = n * probe_count
    r_iota = lax.broadcasted_iota(jnp.int32, (big, big), 0)
    c_iota = lax.broadcasted_iota(jnp.int32, (big, big), 1)
    p_bits = probe_count.bit_length() - 1
    earlier = jnp.where(
        ((r_iota >> p_bits) == (c_iota >> p_bits)) & (c_iota < r_iota), 1.0, 0.0
    ).astype(jnp.bfloat16)
    before = jnp.where(
        lax.broadcasted_iota(jnp.int32, (per_device, per_device), 0)
        < lax.broadcasted_iota(jnp.int32, (per_device, per_device), 1), 1.0, 0.0,
    ).astype(jnp.bfloat16)
    lead = jnp.dot(earlier, hits, preferred_element_type=jnp.float32).astype(jnp.bfloat16)
    ranks = jnp.dot(hits, before, preferred_element_type=jnp.float32) + jnp.dot(
        lead, jnp.ones((per_device, per_device), jnp.bfloat16), preferred_element_type=jnp.float32
    )
    rank = jnp.zeros((probe_count, per_device), jnp.float32)
    for o in range(n):
        rank = jnp.where(target == o, ranks[o * probe_count : (o + 1) * probe_count], rank)
    slot = target * cap + rank.astype(jnp.int32)
    code = local * per_device + lax.broadcasted_iota(jnp.int32, (probe_count, per_device), 1)
    word = (slot << code_bits) | code
    for q in range(per_device):
        slots[q * probe_count : (q + 1) * probe_count, :] = jnp.broadcast_to(
            word[:, q : q + 1], (probe_count, LANES)
        )

    def one_table(b, carry):
        lane = lax.broadcasted_iota(jnp.int32, (pairs, LANES), 1) + b * LANES
        held = slots[...]
        found = jnp.where((held >> code_bits) == lane, held & ((1 << code_bits) - 1), 0)
        ms[me, b] = jnp.sum(found.astype(jnp.float32), axis=0, keepdims=True).astype(jnp.int32)
        return carry

    lax.fori_loop(0, tables, one_table, 0)
    ms[me, tables] = jnp.zeros((1, LANES), jnp.int32)
    ms[me, tables, :, 0:clusters] = cnt_v[...]
    onward(push, me, 2, has_low, has_high)
    live_row = ms[me, tables].astype(jnp.float32)
    cntb[...] = jnp.transpose(jnp.broadcast_to(live_row, (LANES, LANES)))[0:clusters]

    near = jnp.minimum(z, planes - 1 - z)
    long_side = jnp.where(z < planes - 1 - z, 1, -1)

    def plane_of(k):
        both = jnp.where(k % 2 == 1, -1, 1) * ((k + 1) // 2)
        return z + jnp.where(k <= 2 * near, both, long_side * (k - near))

    def relay_z(k, act=push, wait=True):
        p = plane_of(k)
        s = p * 4 + y * 2 + c
        for h in range(3):
            if wait:
                arrive(s, h)
            onward(act, s, h, (p > z) & has_low, (p < z) & has_high)

    def relay_y(k):
        s = plane_of(k) * 4 + (1 - y) * 2 + c
        for h in range(3):
            arrive(s, h)
            push(s, h, 3, c_dev)

    def back_pair(s):
        return (
            pltpu.make_async_remote_copy(
                src_ref=sendb.at[pl.ds(s * cap, cap)], dst_ref=recvb.at[pl.ds(me * cap, cap)],
                send_sem=bsend.at[s], recv_sem=brecv.at[me], device_id={"owner": s},
            ),
            pltpu.make_async_remote_copy(
                src_ref=sends.at[s // 2], dst_ref=recvs.at[me],
                send_sem=ssend.at[s], recv_sem=srecv.at[me], device_id={"owner": s},
            ),
        )

    def compute(k):
        p = plane_of(k)
        base = p * 4
        codes = jnp.concatenate(
            [join(ms[base + 2 * b, me // 2], ms[base + 2 * b + 1, me // 2]) for b in range(2)], axis=1
        )
        cluster = codes >> q_bits
        block_of = lax.broadcasted_iota(jnp.int32, (1, wide), 1) // cap
        source = (codes & (per_device - 1)) + block_of * per_device
        pick = jnp.where(
            lax.broadcasted_iota(jnp.int32, (rows, wide), 0) == source, 1.0, 0.0
        ).astype(jnp.bfloat16)
        rows_v[...] = lax.dot_general(
            pick, qs[pl.ds(base, 4)].reshape(rows, width), (((0,), (0,)), ((), ())),
            preferred_element_type=jnp.float32,
        ).astype(jnp.bfloat16)
        centre = lax.dot_general(
            cent_v[...], rows_v[...], (((1,), (1,)), ((), ())), preferred_element_type=jnp.float32
        )
        mine = lax.broadcasted_iota(jnp.int32, (clusters, wide), 0) == cluster
        term = jnp.sum(jnp.where(mine, centre, 0.0), axis=0, keepdims=True)
        count_of = jnp.concatenate([cntb[...], cntb[...]], axis=1)
        live = jnp.sum(jnp.where(mine, count_of, 0.0), axis=0, keepdims=True).astype(jnp.int32)

        def some_clusters(g, carry):
            @pl.when(k == 0)
            def _():
                for u in range(GROUP):
                    passage_copy(g * GROUP + u).wait()

            tall = GROUP * span
            direct = lax.dot_general(
                pass_v[pl.ds(g * tall, tall)], rows_v[...], (((1,), (1,)), ((), ())),
                preferred_element_type=jnp.float32,
            )
            total = acc[...]
            for u in range(GROUP):
                total = jnp.where(
                    jnp.broadcast_to(cluster, (span, wide)) == g * GROUP + u,
                    direct[u * span : (u + 1) * span], total,
                )
            acc[...] = total
            return carry

        acc[...] = jnp.zeros((span, wide), jnp.float32)
        lax.fori_loop(0, clusters // GROUP, some_clusters, 0)
        place = lax.broadcasted_iota(jnp.int32, (span, wide), 0)
        value = jnp.where(place < live, acc[...] + term, 0.0)
        top = jnp.maximum(jnp.max(jnp.abs(value), axis=0, keepdims=True), 1e-30)
        coded = jnp.round(value * (TOP / top)).astype(jnp.int32)
        packed = (coded[half:] << 16) | (coded[:half] & 0xFFFF)
        sendb[pl.ds(base * cap, wide)] = jnp.transpose(packed)
        unit = top * (1.0 / TOP)
        for b in range(2):
            sends[p * 2 + b] = unit[:, b * LANES : (b + 1) * LANES]
        for i in range(4):
            s = base + i

            @pl.when(s == me)
            def _():
                recvb[pl.ds(me * cap, cap)] = sendb[pl.ds(me * cap, cap)]
                recvs[me] = sends[me // 2]

            @pl.when(s != me)
            def _():
                for copy in back_pair(s):
                    copy.start()

    ahead = 1 + jnp.where(near >= 1, 1, 0)

    def step(k, carry):
        @pl.when((k == 0) & (planes > 1))
        def _():
            relay_z(1)

        @pl.when((k == 0) & (ahead > 1))
        def _():
            relay_z(2)

        @pl.when((k > 0) & (k + ahead < planes))
        def _():
            relay_z(k + ahead)

        relay_y(k)
        p = plane_of(k)
        for h in range(3):
            arrive(p * 4 + y * 2 + (1 - c), h)
            arrive(p * 4 + (1 - y) * 2 + (1 - c), h)
        compute(k)
        return carry

    lax.fori_loop(0, planes, step, 0)

    count_copy = pltpu.make_async_copy(ms.at[:, tables], cnt_s, load_sem.at[0])
    count_copy.start()
    count_copy.wait()

    def one_owner(o, seen):
        for l in range(clusters):
            seen = jnp.where(probe_v[...] == o * clusters + l, cnt_s[o, 0, l], seen)
        return seen

    seen = lax.fori_loop(0, n, one_owner, jnp.zeros((probe_count, per_device), jnp.int32))
    vis_ref[...] = jnp.sum(seen.astype(jnp.float32), axis=0, keepdims=True).astype(jnp.int32)

    def collect(k, carry):
        p = plane_of(k)
        base = p * 4
        for i in range(4):
            s = base + i

            @pl.when(s != me)
            def _():
                for copy in (
                    pltpu.make_async_remote_copy(
                        src_ref=sendb.at[pl.ds(s * cap, cap)], dst_ref=recvb.at[pl.ds(s * cap, cap)],
                        send_sem=bsend.at[s], recv_sem=brecv.at[s], device_id={"owner": c_dev},
                    ),
                    pltpu.make_async_remote_copy(
                        src_ref=sends.at[s // 2], dst_ref=recvs.at[s],
                        send_sem=ssend.at[s], recv_sem=srecv.at[s], device_id={"owner": c_dev},
                    ),
                ):
                    copy.wait_recv()

        units = jnp.concatenate(
            [
                jnp.transpose(jnp.broadcast_to(
                    join(recvs[base + 2 * b], recvs[base + 2 * b + 1]), (LANES, LANES)
                ))
                for b in range(2)
            ],
            axis=0,
        )
        held = recvb[pl.ds(base * cap, wide)]
        value = jnp.concatenate(
            [
                ((held << 16) >> 16).astype(jnp.float32) * units,
                (held >> 16).astype(jnp.float32) * units,
            ],
            axis=1,
        )
        upper_part = value.astype(jnp.bfloat16)
        lower_part = (value - upper_part.astype(jnp.float32)).astype(jnp.bfloat16)
        at = slots[...] >> code_bits
        lane = lax.broadcasted_iota(jnp.int32, (pairs, LANES), 1) + base * cap
        chosen = jnp.concatenate(
            [jnp.where(at == lane + b * LANES, 1.0, 0.0).astype(jnp.bfloat16) for b in range(2)], axis=1
        )
        part = jnp.dot(chosen, upper_part, preferred_element_type=jnp.float32) + jnp.dot(
            chosen, lower_part, preferred_element_type=jnp.float32
        )

        @pl.when(k == 0)
        def _():
            out_ref[...] = part

        @pl.when(k > 0)
        def _():
            out_ref[...] += part

        return carry

    lax.fori_loop(0, planes, collect, 0)

    for h in range(3):
        onward(drain, me, h, has_low, has_high)

    def finish(k, carry):
        @pl.when(k > 0)
        def _():
            relay_z(k, drain, False)

        for h in range(3):
            drain(plane_of(k) * 4 + (1 - y) * 2 + c, h, 3, c_dev)
        return carry

    lax.fori_loop(0, planes, finish, 0)

    def finish_back(s, carry):
        @pl.when(s != me)
        def _():
            for copy in back_pair(s):
                copy.wait_send()

        return carry

    lax.fori_loop(0, n, finish_back, 0)


def fused_body(queries, probes, passages, centroids, counts):
    n = lax.axis_size("owner")
    per_device, probe_count = probes.shape
    clusters, span, width = passages.shape
    cap = 2 * per_device * probe_count // n
    pairs = per_device * probe_count
    tables = n * cap // LANES
    wide = 4 * cap
    vmem = pl.BlockSpec(memory_space=pltpu.VMEM)
    hbm = pl.BlockSpec(memory_space=pltpu.HBM)
    dma = pltpu.SemaphoreType.DMA
    scores, visits = pl.pallas_call(
        lambda *refs: owner_kernel(n, *refs),
        out_shape=(
            jax.ShapeDtypeStruct((pairs, span), jnp.float32),
            jax.ShapeDtypeStruct((1, per_device), jnp.int32),
        ),
        in_specs=[hbm] * 5,
        out_specs=(vmem, vmem),
        scratch_shapes=[
            pltpu.VMEM((clusters * span, width), jnp.bfloat16),
            pltpu.VMEM((n, per_device, width), jnp.bfloat16),
            pltpu.VMEM((clusters, width), jnp.bfloat16),
            pltpu.VMEM((1, clusters), jnp.int32),
            pltpu.VMEM((probe_count, per_device), jnp.int32),
            pltpu.VMEM((n, tables + 1, 1, LANES), jnp.int32),
            pltpu.VMEM((pairs, LANES), jnp.int32),
            pltpu.VMEM((wide, width), jnp.bfloat16),
            pltpu.VMEM((span, wide), jnp.float32),
            pltpu.VMEM((clusters, LANES), jnp.float32),
            pltpu.VMEM((n * cap, LANES), jnp.int32),
            pltpu.VMEM((n // 2, 1, LANES), jnp.float32),
            pltpu.VMEM((n * cap, LANES), jnp.int32),
            pltpu.VMEM((n, 1, LANES), jnp.float32),
            pltpu.SMEM((n, 1, LANES), jnp.int32),
            dma((clusters,)),
            dma((4,)),
            dma((n, 2, 4)),
            dma((n, 4)),
            dma((n, 2)),
            dma((n,)),
            dma((n,)),
            dma((n,)),
            dma((n,)),
            dma((n,)),
        ],
        compiler_params=pltpu.CompilerParams(
            collective_id=0, has_side_effects=True, vmem_limit_bytes=48 * 2**20
        ),
    )(queries, probes.T, passages, centroids, counts.reshape(1, clusters))
    return scores.reshape(per_device, probe_count, span), visits.reshape(per_device)


def power_of_two(value):
    return value > 0 and value & (value - 1) == 0


def body(queries, probes, passages, centroids, counts):
    n = lax.axis_size("owner")
    per_device, probe_count = probes.shape
    clusters, span, width = passages.shape
    cap = 2 * per_device * probe_count // n
    held = 2 * width * (clusters * span + n * per_device)
    fits = (
        n % 8 == 0 and 2 * cap == LANES and n * probe_count == LANES and span == 2 * LANES
        and power_of_two(clusters) and power_of_two(per_device) and power_of_two(probe_count)
        and clusters % GROUP == 0 and 8 <= clusters <= LANES and per_device == cap
        and clusters * per_device * n * cap < 2**23 and width % LANES == 0 and held < 32 * 2**20
    )
    chosen = fused_body if fits else routed_body
    return chosen(queries, probes, passages, centroids, counts)


def solution(mesh):
    in_specs = (
        P(("groups", "owner"), None),
        P(("groups", "owner"), None),
        P("owner", None, None),
        P("owner", None),
        P("owner"),
    )
    out_specs = (P(("groups", "owner"), None, None), P(("groups", "owner")))
    return jax.shard_map(body, mesh=mesh, in_specs=in_specs, out_specs=out_specs, check_vma=False)
```

```python
import jax
import jax.numpy as jnp
from jax import lax
from jax.experimental import pallas as pl
from jax.experimental.pallas import tpu as pltpu
from jax.sharding import PartitionSpec as P


def routed_body(queries, probes, passages, centroids, counts):
    owner_count = lax.axis_size("owner")
    per_device, probe_count = probes.shape
    local_count, block_span, feature_width = passages.shape
    capacity = 2 * per_device * probe_count // owner_count
    pair_count = per_device * probe_count
    passage_blocks = jnp.transpose(passages, (0, 2, 1))
    flat_probes = probes.reshape(-1)
    target_owner = flat_probes // local_count
    target_local = flat_probes % local_count
    owner_hits = (
        target_owner[:, None] == jnp.arange(owner_count, dtype=jnp.int32)[None, :]
    ).astype(jnp.int32)
    slot_rank = jnp.sum((jnp.cumsum(owner_hits, axis=0) - owner_hits) * owner_hits, axis=1)
    slot_index = target_owner * capacity + slot_rank
    pair_ids = jnp.arange(pair_count, dtype=jnp.int32)
    slot_match = slot_index[None, :] == jnp.arange(owner_count * capacity, dtype=jnp.int32)[:, None]
    slot_filled = jnp.any(slot_match, axis=1)
    source_pair = jnp.sum(jnp.where(slot_match, pair_ids[None, :], 0), axis=1)
    send_rows = jnp.where(
        slot_filled[:, None], queries[source_pair // probe_count], jnp.zeros((), jnp.bfloat16)
    )
    send_ids = jnp.where(slot_filled, target_local[source_pair], -1)
    query_rows = lax.all_to_all(
        send_rows.reshape(owner_count, capacity, feature_width),
        "owner",
        split_axis=0,
        concat_axis=0,
        tiled=True,
    )
    cluster_ids = lax.all_to_all(
        send_ids.reshape(owner_count, capacity), "owner", split_axis=0, concat_axis=0, tiled=True
    )
    source_count, slot_count = cluster_ids.shape
    row_total = source_count * slot_count
    flat_rows = query_rows.reshape(row_total, feature_width)
    flat_ids = cluster_ids.reshape(-1)
    group_ids = jnp.where(flat_ids < 0, 0, flat_ids).astype(jnp.int32)
    cluster_pick = flat_ids[:, None] == jnp.arange(local_count, dtype=jnp.int32)[None, :]
    live_sizes = jnp.sum(jnp.where(cluster_pick, counts[None, :], 0), axis=1)
    group_pick = group_ids[:, None] == jnp.arange(local_count, dtype=jnp.int32)[None, :]
    group_sizes = jnp.sum(group_pick.astype(jnp.int32), axis=0)
    order = jnp.argsort(group_ids, stable=True)
    undo_order = jnp.argsort(order, stable=True)
    sorted_rows = flat_rows[order]
    sorted_scores = lax.ragged_dot(
        sorted_rows, passage_blocks, group_sizes, preferred_element_type=jnp.float32
    )
    own_scores = sorted_scores[undo_order]
    centre_term = jnp.einsum(
        "rd,rd->r", flat_rows, centroids[group_ids], preferred_element_type=jnp.float32
    )
    live_mask = jnp.arange(block_span, dtype=jnp.int32)[None, :] < live_sizes[:, None]
    masked_scores = jnp.where(live_mask, own_scores + centre_term[:, None], 0.0)
    back_scores = lax.all_to_all(
        masked_scores.reshape(source_count, slot_count, block_span),
        "owner",
        split_axis=0,
        concat_axis=0,
        tiled=True,
    )
    back_sizes = lax.all_to_all(
        live_sizes.astype(jnp.float32).reshape(source_count, slot_count),
        "owner",
        split_axis=0,
        concat_axis=0,
        tiled=True,
    )
    flat_scores = back_scores.reshape(owner_count * capacity, block_span)
    scores = flat_scores[slot_index].reshape(per_device, probe_count, block_span)
    pair_sizes = back_sizes.reshape(-1)[slot_index].reshape(per_device, probe_count)
    visits = jnp.sum(pair_sizes, axis=1).astype(jnp.int32)
    return (scores, visits)


LANES = 128
GROUP = 8
TOP = 32767.0


def owner_kernel(
    n, q_hbm, probe_hbm, pass_hbm, cent_hbm, cnt_hbm,
    out_ref, vis_ref,
    pass_v, qs, centre_v, cnt_v, probe_v, ms, slots, rows_v, acc, cntb, sendb, sends, recvb, recvs, cnt_s,
    pass_sem, load_sem, qsend, msend, qrecv, mrecv, bsend, ssend, brecv, srecv,
):
    clusters, width = cent_hbm.shape
    span = pass_hbm.shape[1]
    tall = GROUP * span
    probe_count, per_device = probe_v.shape
    pairs = probe_count * per_device
    planes = n // 4
    rows = 4 * per_device
    tables = ms.shape[1] - 1
    cap = LANES // 2
    wide = 4 * cap
    half = span // 2
    piece = per_device // 2
    code_bits = (clusters * per_device).bit_length() - 1
    q_bits = per_device.bit_length() - 1
    cl_bits = clusters.bit_length() - 1
    me = lax.axis_index("owner")
    z = me // 4
    y = (me // 2) % 2
    c = me % 2
    y_dev = z * 4 + (1 - y) * 2 + c
    c_dev = z * 4 + y * 2 + (1 - c)
    has_low = z > 0
    has_high = z < planes - 1

    loads = [
        pltpu.make_async_copy(q_hbm, qs.at[me], load_sem.at[0]),
        pltpu.make_async_copy(probe_hbm, probe_v, load_sem.at[1]),
        pltpu.make_async_copy(cnt_hbm, cnt_v, load_sem.at[2]),
    ] + [
        pltpu.make_async_copy(cent_hbm, pass_v.at[g, pl.ds(tall, clusters)], load_sem.at[3 + g])
        for g in range(clusters // GROUP)
    ]
    for copy in loads:
        copy.start()

    barrier = pltpu.get_barrier_semaphore()

    def greet(dev):
        pl.semaphore_signal(barrier, inc=1, device_id={"owner": dev})

    greet(y_dev)
    greet(c_dev)

    @pl.when(has_low)
    def _():
        greet(me - 4)

    @pl.when(has_high)
    def _():
        greet(me + 4)

    def passage_copy(k):
        return pltpu.make_async_copy(pass_hbm.at[k], pass_v.at[k // GROUP, pl.ds((k % GROUP) * span, span)], pass_sem.at[k])

    for k in range(clusters):
        passage_copy(k).start()

    loads[0].wait()
    pl.semaphore_wait(barrier, 2 + jnp.where(has_low, 1, 0) + jnp.where(has_high, 1, 0))

    def chunk(s, h, target, dev):
        if h == 2:
            return pltpu.make_async_remote_copy(
                src_ref=ms.at[s], dst_ref=ms.at[s],
                send_sem=msend.at[s, target], recv_sem=mrecv.at[s], device_id={"owner": dev},
            )
        cut = pl.ds(h * piece, piece)
        return pltpu.make_async_remote_copy(
            src_ref=qs.at[s, cut], dst_ref=qs.at[s, cut],
            send_sem=qsend.at[s, h, target], recv_sem=qrecv.at[s, h], device_id={"owner": dev},
        )

    def push(s, h, target, dev):
        chunk(s, h, target, dev).start()

    def drain(s, h, target, dev):
        chunk(s, h, target, dev).wait_send()

    def arrive(s, h):
        chunk(s, h, 0, c_dev).wait_recv()

    def onward(act, s, h, low, high):
        @pl.when(low)
        def _():
            act(s, h, 0, me - 4)

        @pl.when(high)
        def _():
            act(s, h, 1, me + 4)

        act(s, h, 2, y_dev)
        act(s, h, 3, c_dev)

    onward(push, me, 0, has_low, has_high)

    for copy in loads[1:]:
        copy.wait()

    def lower(row):
        return jnp.where(c == 1, pltpu.roll(row, cap, 1), row)

    def upper(row):
        return jnp.where(c == 1, row, pltpu.roll(row, cap, 1))

    lane_row = lax.broadcasted_iota(jnp.int32, (8, LANES), 1)

    def join(first, second):
        first = jnp.broadcast_to(first, (8, LANES))
        second = jnp.broadcast_to(second, (8, LANES))
        return jnp.where(lane_row < cap, lower(first), upper(second))[0:1]

    probes = probe_v[...]
    target = probes >> cl_bits
    local = probes & (clusters - 1)
    hits = jnp.concatenate(
        [jnp.where(target == o, 1.0, 0.0).astype(jnp.float32) for o in range(n)], axis=0
    ).astype(jnp.bfloat16)
    big = n * probe_count
    r_iota = lax.broadcasted_iota(jnp.int32, (big, big), 0)
    c_iota = lax.broadcasted_iota(jnp.int32, (big, big), 1)
    p_bits = probe_count.bit_length() - 1
    earlier = jnp.where(
        ((r_iota >> p_bits) == (c_iota >> p_bits)) & (c_iota < r_iota), 1.0, 0.0
    ).astype(jnp.bfloat16)
    before = jnp.where(
        lax.broadcasted_iota(jnp.int32, (per_device, per_device), 0)
        < lax.broadcasted_iota(jnp.int32, (per_device, per_device), 1), 1.0, 0.0,
    ).astype(jnp.bfloat16)
    lead = jnp.dot(earlier, hits, preferred_element_type=jnp.float32).astype(jnp.bfloat16)
    ranks = jnp.dot(hits, before, preferred_element_type=jnp.float32) + jnp.dot(
        lead, jnp.ones((per_device, per_device), jnp.bfloat16), preferred_element_type=jnp.float32
    )
    rank = jnp.zeros((probe_count, per_device), jnp.float32)
    for o in range(n):
        rank = jnp.where(target == o, ranks[o * probe_count : (o + 1) * probe_count], rank)
    slot = target * cap + rank.astype(jnp.int32)
    code = local * per_device + lax.broadcasted_iota(jnp.int32, (probe_count, per_device), 1)
    word = (slot << code_bits) | code
    for q in range(per_device):
        slots[q * probe_count : (q + 1) * probe_count, :] = jnp.broadcast_to(
            word[:, q : q + 1], (probe_count, LANES)
        )

    def one_table(b, carry):
        lane = lax.broadcasted_iota(jnp.int32, (pairs, LANES), 1) + b * LANES
        held = slots[...]
        found = jnp.where((held >> code_bits) == lane, held & ((1 << code_bits) - 1), 0)
        ms[me, b] = jnp.sum(found.astype(jnp.float32), axis=0, keepdims=True).astype(jnp.int32)
        return carry

    lax.fori_loop(0, tables, one_table, 0)
    ms[me, tables] = jnp.zeros((1, LANES), jnp.int32)
    ms[me, tables, :, 0:clusters] = cnt_v[...]
    onward(push, me, 2, has_low, has_high)
    onward(push, me, 1, has_low, has_high)
    live_row = ms[me, tables].astype(jnp.float32)
    cntb[...] = jnp.transpose(jnp.broadcast_to(live_row, (LANES, LANES)))[0:clusters]

    near = jnp.minimum(z, planes - 1 - z)
    long_side = jnp.where(z < planes - 1 - z, 1, -1)

    far = planes - 1 - near

    def plane_of(k):
        return z + long_side * jnp.where(k <= far, k, far - k)

    def collect_of(k):
        ends = jnp.where(k == 1, 2, jnp.where(k == 2, 1, k))
        inner = jnp.where(k == 1, -1, jnp.where(k > 1, k - 1, 0))
        return z + long_side * jnp.where(near == 0, ends, inner)

    def pick_of(u, values):
        found = values[0]
        for at in range(1, len(values)):
            found = jnp.where(u == at, values[at], found)
        return found

    def chips_of(u):
        inner = near > 0
        first = pick_of(u, (0, 2, jnp.where(inner, 0, 3), jnp.where(inner, 3, 2)))
        first_far = pick_of(u, (0, 0, jnp.where(inner, 1, 0), jnp.where(inner, 0, 1)))
        second = pick_of(u, (1, jnp.where(inner, 1, 0), jnp.where(inner, 2, 1), 3))
        second_far = jnp.where(u == 0, 0, 1)

        def chip(k, other):
            return plane_of(k) * 2 + jnp.where(other == 1, 1 - y, y)

        return chip(first, first_far), chip(second, second_far)

    def along(k):
        return plane_of(k) * 4 + y * 2 + c

    def forward_z(k, h, act=push, wait=True):
        p = plane_of(k)
        if wait:
            arrive(along(k), h)

        @pl.when((p > z) & has_low)
        def _():
            act(along(k), h, 0, me - 4)

        @pl.when((p < z) & has_high)
        def _():
            act(along(k), h, 1, me + 4)

    def forward_y(k, h, act=push):
        act(along(k), h, 2, y_dev)

    def forward_c(k, h, act=push):
        act(along(k), h, 3, c_dev)

    def forward_plane(k, h, act=push):
        forward_y(k, h, act)
        forward_c(k, h, act)

    def relay_y(k, h):
        s = plane_of(k) * 4 + (1 - y) * 2 + c
        arrive(s, h)
        push(s, h, 3, c_dev)

    def service(u, pieces):
        for h in pieces:
            @pl.when(u + 2 <= far)
            def _():
                forward_z(u + 2, h)
                forward_plane(u + 2, h)

            @pl.when(u + 1 < planes)
            def _():
                relay_y(u + 1, h)

    def back_pair(s):
        return (
            pltpu.make_async_remote_copy(
                src_ref=sendb.at[pl.ds(s * cap, cap)], dst_ref=recvb.at[pl.ds(me * cap, cap)],
                send_sem=bsend.at[s], recv_sem=brecv.at[me], device_id={"owner": s},
            ),
            pltpu.make_async_remote_copy(
                src_ref=sends.at[s // 2], dst_ref=recvs.at[me],
                send_sem=ssend.at[s], recv_sem=srecv.at[me], device_id={"owner": s},
            ),
        )

    def compute(k):
        chips = chips_of(k)
        codes = jnp.concatenate(
            [join(ms[2 * chip, me // 2], ms[2 * chip + 1, me // 2]) for chip in chips], axis=1
        )
        cluster = codes >> q_bits
        block_of = lax.broadcasted_iota(jnp.int32, (1, wide), 1) // cap
        source = (codes & (per_device - 1)) + block_of * per_device
        pick = jnp.where(
            lax.broadcasted_iota(jnp.int32, (rows, wide), 0) == source, 1.0, 0.0
        ).astype(jnp.bfloat16)
        block = jnp.concatenate(
            [qs[pl.ds(2 * chip, 2)].reshape(2 * per_device, width) for chip in chips], axis=0
        )
        rows_v[...] = lax.dot_general(
            pick, block, (((0,), (0,)), ((), ())),
            preferred_element_type=jnp.float32,
        ).astype(jnp.bfloat16)
        def some_clusters(g, carry):
            @pl.when(k == 0)
            def _():
                for u in range(GROUP):
                    passage_copy(g * GROUP + u).wait()

            direct = lax.dot_general(
                pass_v[g], rows_v[...], (((1,), (1,)), ((), ())),
                preferred_element_type=jnp.float32,
            )
            total = acc[...]
            for u in range(GROUP):
                total = jnp.where(
                    jnp.broadcast_to(cluster, (span, wide)) == g * GROUP + u,
                    direct[u * span : (u + 1) * span], total,
                )
            acc[...] = total
            centre_v[...] = direct[tall:]

            @pl.when(g == 0)
            def _():
                service(k, (0, 2))

                @pl.when(k > 0)
                def _():
                    service(k, (1,))

            @pl.when(g == 1)
            def _():
                @pl.when(k == 0)
                def _():
                    service(k, (1,))

                @pl.when((k == 0) & (near > 0))
                def _():
                    for h in (0, 2, 1):
                        forward_y(planes - 1, h)

            return carry

        acc[...] = jnp.zeros((span, wide), jnp.float32)
        lax.fori_loop(0, clusters // GROUP, some_clusters, 0)
        mine = lax.broadcasted_iota(jnp.int32, (clusters, wide), 0) == cluster
        term = jnp.sum(jnp.where(mine, centre_v[...], 0.0), axis=0, keepdims=True)
        count_of = jnp.concatenate([cntb[...], cntb[...]], axis=1)
        live = jnp.sum(jnp.where(mine, count_of, 0.0), axis=0, keepdims=True).astype(jnp.int32)
        place = lax.broadcasted_iota(jnp.int32, (span, wide), 0)
        value = jnp.where(place < live, acc[...] + term, 0.0)
        top = jnp.maximum(jnp.max(jnp.abs(value), axis=0, keepdims=True), 1e-30)
        coded = jnp.round(value * (TOP / top)).astype(jnp.int32)
        packed = (coded[half:] << 16) | (coded[:half] & 0xFFFF)
        turned = jnp.transpose(packed)
        unit = top * (1.0 / TOP)
        for b, chip in enumerate(chips):
            sendb[pl.ds(2 * chip * cap, LANES)] = turned[b * LANES : (b + 1) * LANES]
            sends[chip] = unit[:, b * LANES : (b + 1) * LANES]
        for i in range(4):
            s = 2 * chips[i // 2] + i % 2

            @pl.when(s == me)
            def _():
                recvb[pl.ds(me * cap, cap)] = sendb[pl.ds(me * cap, cap)]
                recvs[me] = sends[me // 2]

            @pl.when(s != me)
            def _():
                for copy in back_pair(s):
                    copy.start()

    for h in (0, 2, 1):
        forward_z(1, h)
        forward_plane(1, h)

        @pl.when(near > 0)
        def _():
            forward_z(planes - 1, h)
            forward_c(planes - 1, h)

        relay_y(0, h)

    count_copy = pltpu.make_async_copy(ms.at[:, tables], cnt_s, load_sem.at[0])

    def step(k, carry):
        for chip in chips_of(k):
            for h in range(3):
                arrive(2 * chip + (1 - c), h)

        @pl.when(k == planes - 1)
        def _():
            count_copy.start()

        compute(k)
        return carry

    lax.fori_loop(0, planes, step, 0)

    count_copy.wait()

    def one_owner(o, seen):
        for l in range(clusters):
            seen = jnp.where(probe_v[...] == o * clusters + l, cnt_s[o, 0, l], seen)
        return seen

    seen = lax.fori_loop(0, n, one_owner, jnp.zeros((probe_count, per_device), jnp.int32))
    vis_ref[...] = jnp.sum(seen.astype(jnp.float32), axis=0, keepdims=True).astype(jnp.int32)

    def collect(k, carry):
        p = collect_of(k)
        base = p * 4
        for i in range(4):
            s = base + i

            @pl.when(s != me)
            def _():
                for copy in (
                    pltpu.make_async_remote_copy(
                        src_ref=sendb.at[pl.ds(s * cap, cap)], dst_ref=recvb.at[pl.ds(s * cap, cap)],
                        send_sem=bsend.at[s], recv_sem=brecv.at[s], device_id={"owner": c_dev},
                    ),
                    pltpu.make_async_remote_copy(
                        src_ref=sends.at[s // 2], dst_ref=recvs.at[s],
                        send_sem=ssend.at[s], recv_sem=srecv.at[s], device_id={"owner": c_dev},
                    ),
                ):
                    copy.wait_recv()

        units = jnp.concatenate(
            [
                jnp.transpose(jnp.broadcast_to(
                    join(recvs[base + 2 * b], recvs[base + 2 * b + 1]), (LANES, LANES)
                ))
                for b in range(2)
            ],
            axis=0,
        )
        held = recvb[pl.ds(base * cap, wide)]
        value = jnp.concatenate(
            [
                ((held << 16) >> 16).astype(jnp.float32) * units,
                (held >> 16).astype(jnp.float32) * units,
            ],
            axis=1,
        )
        upper_part = value.astype(jnp.bfloat16)
        lower_part = (value - upper_part.astype(jnp.float32)).astype(jnp.bfloat16)
        at = slots[...] >> code_bits
        lane = lax.broadcasted_iota(jnp.int32, (pairs, LANES), 1) + base * cap
        chosen = jnp.concatenate(
            [jnp.where(at == lane + b * LANES, 1.0, 0.0).astype(jnp.bfloat16) for b in range(2)], axis=1
        )
        part = jnp.dot(chosen, upper_part, preferred_element_type=jnp.float32) + jnp.dot(
            chosen, lower_part, preferred_element_type=jnp.float32
        )

        @pl.when(k == 0)
        def _():
            out_ref[...] = part

        @pl.when(k > 0)
        def _():
            out_ref[...] += part

        return carry

    lax.fori_loop(0, planes, collect, 0)

    for h in range(3):
        onward(drain, me, h, has_low, has_high)

    def finish(k, carry):
        @pl.when(k > 0)
        def _():
            for h in range(3):
                forward_z(k, h, drain, False)
                forward_plane(k, h, drain)

        for h in range(3):
            drain(plane_of(k) * 4 + (1 - y) * 2 + c, h, 3, c_dev)
        return carry

    lax.fori_loop(0, planes, finish, 0)

    def finish_back(s, carry):
        @pl.when(s != me)
        def _():
            for copy in back_pair(s):
                copy.wait_send()

        return carry

    lax.fori_loop(0, n, finish_back, 0)


def fused_body(queries, probes, passages, centroids, counts):
    n = lax.axis_size("owner")
    per_device, probe_count = probes.shape
    clusters, span, width = passages.shape
    cap = 2 * per_device * probe_count // n
    pairs = per_device * probe_count
    tables = n * cap // LANES
    wide = 4 * cap
    vmem = pl.BlockSpec(memory_space=pltpu.VMEM)
    hbm = pl.BlockSpec(memory_space=pltpu.HBM)
    dma = pltpu.SemaphoreType.DMA
    scores, visits = pl.pallas_call(
        lambda *refs: owner_kernel(n, *refs),
        out_shape=(
            jax.ShapeDtypeStruct((pairs, span), jnp.float32),
            jax.ShapeDtypeStruct((1, per_device), jnp.int32),
        ),
        in_specs=[hbm] * 5,
        out_specs=(vmem, vmem),
        scratch_shapes=[
            pltpu.VMEM((clusters // GROUP, GROUP * span + clusters, width), jnp.bfloat16),
            pltpu.VMEM((n, per_device, width), jnp.bfloat16),
            pltpu.VMEM((clusters, wide), jnp.float32),
            pltpu.VMEM((1, clusters), jnp.int32),
            pltpu.VMEM((probe_count, per_device), jnp.int32),
            pltpu.VMEM((n, tables + 1, 1, LANES), jnp.int32),
            pltpu.VMEM((pairs, LANES), jnp.int32),
            pltpu.VMEM((wide, width), jnp.bfloat16),
            pltpu.VMEM((span, wide), jnp.float32),
            pltpu.VMEM((clusters, LANES), jnp.float32),
            pltpu.VMEM((n * cap, LANES), jnp.int32),
            pltpu.VMEM((n // 2, 1, LANES), jnp.float32),
            pltpu.VMEM((n * cap, LANES), jnp.int32),
            pltpu.VMEM((n, 1, LANES), jnp.float32),
            pltpu.SMEM((n, 1, LANES), jnp.int32),
            dma((clusters,)),
            dma((3 + clusters // GROUP,)),
            dma((n, 2, 4)),
            dma((n, 4)),
            dma((n, 2)),
            dma((n,)),
            dma((n,)),
            dma((n,)),
            dma((n,)),
            dma((n,)),
        ],
        compiler_params=pltpu.CompilerParams(
            collective_id=0, has_side_effects=True, vmem_limit_bytes=48 * 2**20
        ),
    )(*[pltpu.with_memory_space_constraint(v, pltpu.HBM) for v in (queries, probes.T, passages, centroids, counts.reshape(1, clusters))])
    return scores.reshape(per_device, probe_count, span), visits.reshape(per_device)


def power_of_two(value):
    return value > 0 and value & (value - 1) == 0


def body(queries, probes, passages, centroids, counts):
    n = lax.axis_size("owner")
    per_device, probe_count = probes.shape
    clusters, span, width = passages.shape
    cap = 2 * per_device * probe_count // n
    held = 2 * width * (clusters * span + n * per_device)
    fits = (
        n == 16 and clusters % 16 == 0 and 2 * cap == LANES and n * probe_count == LANES and span == 2 * LANES
        and power_of_two(clusters) and power_of_two(per_device) and power_of_two(probe_count)
        and clusters % GROUP == 0 and clusters <= LANES and per_device == cap
        and clusters * per_device * n * cap < 2**23 and width % LANES == 0 and held < 32 * 2**20
    )
    chosen = fused_body if fits else routed_body
    return chosen(queries, probes, passages, centroids, counts)


def solution(mesh):
    in_specs = (
        P(("groups", "owner"), None),
        P(("groups", "owner"), None),
        P("owner", None, None),
        P("owner", None),
        P("owner"),
    )
    out_specs = (P(("groups", "owner"), None, None), P(("groups", "owner")))
    return jax.shard_map(body, mesh=mesh, in_specs=in_specs, out_specs=out_specs, check_vma=False)
```

```python
import jax
import jax.numpy as jnp
from jax import lax
from jax.experimental import pallas as pl
from jax.experimental.pallas import tpu as pltpu
from jax.sharding import PartitionSpec as P


def routed_body(queries, probes, passages, centroids, counts):
    owner_count = lax.axis_size("owner")
    per_device, probe_count = probes.shape
    local_count, block_span, feature_width = passages.shape
    capacity = 2 * per_device * probe_count // owner_count
    pair_count = per_device * probe_count
    passage_blocks = jnp.transpose(passages, (0, 2, 1))
    flat_probes = probes.reshape(-1)
    target_owner = flat_probes // local_count
    target_local = flat_probes % local_count
    owner_hits = (
        target_owner[:, None] == jnp.arange(owner_count, dtype=jnp.int32)[None, :]
    ).astype(jnp.int32)
    slot_rank = jnp.sum((jnp.cumsum(owner_hits, axis=0) - owner_hits) * owner_hits, axis=1)
    slot_index = target_owner * capacity + slot_rank
    pair_ids = jnp.arange(pair_count, dtype=jnp.int32)
    slot_match = slot_index[None, :] == jnp.arange(owner_count * capacity, dtype=jnp.int32)[:, None]
    slot_filled = jnp.any(slot_match, axis=1)
    source_pair = jnp.sum(jnp.where(slot_match, pair_ids[None, :], 0), axis=1)
    send_rows = jnp.where(
        slot_filled[:, None], queries[source_pair // probe_count], jnp.zeros((), jnp.bfloat16)
    )
    send_ids = jnp.where(slot_filled, target_local[source_pair], -1)
    query_rows = lax.all_to_all(
        send_rows.reshape(owner_count, capacity, feature_width),
        "owner",
        split_axis=0,
        concat_axis=0,
        tiled=True,
    )
    cluster_ids = lax.all_to_all(
        send_ids.reshape(owner_count, capacity), "owner", split_axis=0, concat_axis=0, tiled=True
    )
    source_count, slot_count = cluster_ids.shape
    row_total = source_count * slot_count
    flat_rows = query_rows.reshape(row_total, feature_width)
    flat_ids = cluster_ids.reshape(-1)
    group_ids = jnp.where(flat_ids < 0, 0, flat_ids).astype(jnp.int32)
    cluster_pick = flat_ids[:, None] == jnp.arange(local_count, dtype=jnp.int32)[None, :]
    live_sizes = jnp.sum(jnp.where(cluster_pick, counts[None, :], 0), axis=1)
    group_pick = group_ids[:, None] == jnp.arange(local_count, dtype=jnp.int32)[None, :]
    group_sizes = jnp.sum(group_pick.astype(jnp.int32), axis=0)
    order = jnp.argsort(group_ids, stable=True)
    undo_order = jnp.argsort(order, stable=True)
    sorted_rows = flat_rows[order]
    sorted_scores = lax.ragged_dot(
        sorted_rows, passage_blocks, group_sizes, preferred_element_type=jnp.float32
    )
    own_scores = sorted_scores[undo_order]
    centre_term = jnp.einsum(
        "rd,rd->r", flat_rows, centroids[group_ids], preferred_element_type=jnp.float32
    )
    live_mask = jnp.arange(block_span, dtype=jnp.int32)[None, :] < live_sizes[:, None]
    masked_scores = jnp.where(live_mask, own_scores + centre_term[:, None], 0.0)
    back_scores = lax.all_to_all(
        masked_scores.reshape(source_count, slot_count, block_span),
        "owner",
        split_axis=0,
        concat_axis=0,
        tiled=True,
    )
    back_sizes = lax.all_to_all(
        live_sizes.astype(jnp.float32).reshape(source_count, slot_count),
        "owner",
        split_axis=0,
        concat_axis=0,
        tiled=True,
    )
    flat_scores = back_scores.reshape(owner_count * capacity, block_span)
    scores = flat_scores[slot_index].reshape(per_device, probe_count, block_span)
    pair_sizes = back_sizes.reshape(-1)[slot_index].reshape(per_device, probe_count)
    visits = jnp.sum(pair_sizes, axis=1).astype(jnp.int32)
    return (scores, visits)


LANES = 128
TOP = 32767.0


def owner_kernel(
    n, q_hbm, probe_hbm, pass_hbm, cent_hbm, cnt_hbm,
    out_ref, vis_ref,
    pass_v, qs, cnt_v, probe_v, ms, slots, rows_v, acc, cntb, sendb, sends, recvb, recvs, cnt_s,
    pass_sem, load_sem, qsend, msend, qrecv, mrecv, bsend, ssend, brecv, srecv,
):
    clusters, width = cent_hbm.shape
    span = pass_hbm.shape[1]
    probe_count, per_device = probe_v.shape
    pairs = probe_count * per_device
    planes = n // 4
    rows = 4 * per_device
    tables = ms.shape[1] - 1
    cap = LANES // 2
    wide = 4 * cap
    half = span // 2
    short = cap // 2
    piece = per_device // 2
    code_bits = (clusters * per_device).bit_length() - 1
    q_bits = per_device.bit_length() - 1
    cl_bits = clusters.bit_length() - 1
    me = lax.axis_index("owner")
    z = me // 4
    y = (me // 2) % 2
    c = me % 2
    y_dev = z * 4 + (1 - y) * 2 + c
    c_dev = z * 4 + y * 2 + (1 - c)
    has_low = z > 0
    has_high = z < planes - 1

    loads = [
        pltpu.make_async_copy(q_hbm, qs.at[me], load_sem.at[0]),
        pltpu.make_async_copy(probe_hbm, probe_v, load_sem.at[1]),
        pltpu.make_async_copy(cnt_hbm, cnt_v, load_sem.at[2]),
    ]
    for copy in loads:
        copy.start()

    barrier = pltpu.get_barrier_semaphore()

    def greet(dev):
        pl.semaphore_signal(barrier, inc=1, device_id={"owner": dev})

    greet(y_dev)
    greet(c_dev)

    @pl.when(has_low)
    def _():
        greet(me - 4)

    @pl.when(has_high)
    def _():
        greet(me + 4)

    def passage_copies(g):
        return [
            pltpu.make_async_copy(
                pass_hbm.at[k, pl.ds(g * half, half)], pass_v.at[g, pl.ds(k * half, half)], pass_sem.at[g]
            )
            for k in range(clusters)
        ] + [
            pltpu.make_async_copy(cent_hbm, pass_v.at[g, pl.ds(clusters * half, clusters)], pass_sem.at[g])
        ]

    for g in range(2):
        for copy in passage_copies(g):
            copy.start()

    loads[0].wait()
    pl.semaphore_wait(barrier, 2 + jnp.where(has_low, 1, 0) + jnp.where(has_high, 1, 0))

    def chunk(s, h, target, dev):
        if h == 2:
            return pltpu.make_async_remote_copy(
                src_ref=ms.at[s], dst_ref=ms.at[s],
                send_sem=msend.at[max(target - 1, 0)], recv_sem=mrecv.at[s], device_id={"owner": dev},
            )
        cut = pl.ds(h * piece, piece)
        return pltpu.make_async_remote_copy(
            src_ref=qs.at[s, cut], dst_ref=qs.at[s, cut],
            send_sem=qsend.at[max(target - 1, 0)], recv_sem=qrecv.at[s, h], device_id={"owner": dev},
        )

    def push(s, h, target, dev):
        chunk(s, h, target, dev).start()

    def drain(way, blocks):
        for ref, sem in ((qs, qsend), (ms, msend)):
            pltpu.make_async_remote_copy(
                src_ref=ref.at[pl.ds(0, blocks)], dst_ref=ref.at[pl.ds(0, blocks)],
                send_sem=sem.at[way], recv_sem=mrecv.at[0], device_id={"owner": c_dev},
            ).wait_send()

    def arrive(s, h):
        chunk(s, h, 0, c_dev).wait_recv()

    def onward(act, s, h, low, high):
        @pl.when(low)
        def _():
            act(s, h, 0, me - 4)

        @pl.when(high)
        def _():
            act(s, h, 1, me + 4)

        act(s, h, 2, y_dev)
        act(s, h, 3, c_dev)

    onward(push, me, 0, has_low, has_high)

    for copy in loads[1:]:
        copy.wait()

    def lower(row):
        return jnp.where(c == 1, pltpu.roll(row, cap, 1), row)

    def upper(row):
        return jnp.where(c == 1, row, pltpu.roll(row, cap, 1))

    lane_row = lax.broadcasted_iota(jnp.int32, (8, LANES), 1)

    def join(first, second):
        first = jnp.broadcast_to(first, (8, LANES))
        second = jnp.broadcast_to(second, (8, LANES))
        return jnp.where(lane_row < cap, lower(first), upper(second))[0:1]

    probes = probe_v[...]
    target = probes >> cl_bits
    local = probes & (clusters - 1)
    hits = jnp.concatenate(
        [jnp.where(target == o, 1.0, 0.0).astype(jnp.float32) for o in range(n)], axis=0
    ).astype(jnp.bfloat16)
    big = n * probe_count
    r_iota = lax.broadcasted_iota(jnp.int32, (big, big), 0)
    c_iota = lax.broadcasted_iota(jnp.int32, (big, big), 1)
    p_bits = probe_count.bit_length() - 1
    earlier = jnp.where(
        ((r_iota >> p_bits) == (c_iota >> p_bits)) & (c_iota < r_iota), 1.0, 0.0
    ).astype(jnp.bfloat16)
    before = jnp.where(
        lax.broadcasted_iota(jnp.int32, (per_device, per_device), 0)
        < lax.broadcasted_iota(jnp.int32, (per_device, per_device), 1), 1.0, 0.0,
    ).astype(jnp.bfloat16)
    lead = jnp.dot(earlier, hits, preferred_element_type=jnp.float32).astype(jnp.bfloat16)
    ranks = jnp.dot(hits, before, preferred_element_type=jnp.float32) + jnp.dot(
        lead, jnp.ones((per_device, per_device), jnp.bfloat16), preferred_element_type=jnp.float32
    )
    rank = jnp.zeros((probe_count, per_device), jnp.float32)
    for o in range(n):
        rank = jnp.where(target == o, ranks[o * probe_count : (o + 1) * probe_count], rank)
    slot = target * cap + rank.astype(jnp.int32)
    code = local * per_device + lax.broadcasted_iota(jnp.int32, (probe_count, per_device), 1)
    word = (slot << code_bits) | code
    for q in range(per_device):
        slots[q * probe_count : (q + 1) * probe_count, :] = jnp.broadcast_to(
            word[:, q : q + 1], (probe_count, LANES)
        )

    def one_table(b, carry):
        lane = lax.broadcasted_iota(jnp.int32, (pairs, LANES), 1) + b * LANES
        held = slots[...]
        found = jnp.where((held >> code_bits) == lane, held & ((1 << code_bits) - 1), 0)
        ms[me, b] = jnp.sum(found.astype(jnp.float32), axis=0, keepdims=True).astype(jnp.int32)
        return carry

    lax.fori_loop(0, tables, one_table, 0)
    ms[me, tables] = jnp.zeros((1, LANES), jnp.int32)
    ms[me, tables, :, 0:clusters] = cnt_v[...]
    onward(push, me, 2, has_low, has_high)
    onward(push, me, 1, has_low, has_high)
    live_row = ms[me, tables].astype(jnp.float32)
    cntb[...] = jnp.transpose(jnp.broadcast_to(live_row, (LANES, LANES)))[0:clusters]

    near = jnp.minimum(z, planes - 1 - z)
    long_side = jnp.where(z < planes - 1 - z, 1, -1)

    far = planes - 1 - near

    def plane_of(k):
        return z + long_side * jnp.where(k <= far, k, far - k)

    def collect_of(k):
        ends = jnp.where(k == 1, 2, jnp.where(k == 2, 1, k))
        inner = jnp.where(k == 1, -1, jnp.where(k > 1, k - 1, 0))
        return z + long_side * jnp.where(near == 0, ends, inner)

    def pick_of(u, values):
        found = values[0]
        for at in range(1, len(values)):
            found = jnp.where(u == at, values[at], found)
        return found

    def chips_of(u):
        inner = near > 0
        first = pick_of(u, (0, 2, jnp.where(inner, 0, 3), jnp.where(inner, 3, 2)))
        first_far = pick_of(u, (0, 0, jnp.where(inner, 1, 0), jnp.where(inner, 0, 1)))
        second = pick_of(u, (1, jnp.where(inner, 1, 0), jnp.where(inner, 2, 1), 3))
        second_far = jnp.where(u == 0, 0, 1)

        def chip(k, other):
            return plane_of(k) * 2 + jnp.where(other == 1, 1 - y, y)

        return chip(first, first_far), chip(second, second_far)

    def along(k):
        return plane_of(k) * 4 + y * 2 + c

    def forward_z(k, h, act=push, wait=True):
        p = plane_of(k)
        if wait:
            arrive(along(k), h)

        @pl.when((p > z) & has_low)
        def _():
            act(along(k), h, 0, me - 4)

        @pl.when((p < z) & has_high)
        def _():
            act(along(k), h, 1, me + 4)

    def forward_y(k, h, act=push):
        act(along(k), h, 2, y_dev)

    def forward_c(k, h, act=push):
        act(along(k), h, 3, c_dev)

    def forward_plane(k, h, act=push):
        forward_y(k, h, act)
        forward_c(k, h, act)

    def relay_y(k, h):
        s = plane_of(k) * 4 + (1 - y) * 2 + c
        arrive(s, h)
        push(s, h, 3, c_dev)

    def service(u, pieces):
        for h in pieces:
            @pl.when(u + 2 <= far)
            def _():
                forward_z(u + 2, h)
                forward_plane(u + 2, h)

            @pl.when(u + 1 < planes)
            def _():
                relay_y(u + 1, h)

    def back_pair(g, s):
        return (
            pltpu.make_async_remote_copy(
                src_ref=sendb.at[g, pl.ds(s * short, short)],
                dst_ref=recvb.at[g, pl.ds(me * short, short)],
                send_sem=bsend.at[g], recv_sem=brecv.at[z], device_id={"owner": s},
            ),
            pltpu.make_async_remote_copy(
                src_ref=sends.at[g, s], dst_ref=recvs.at[g, me],
                send_sem=ssend.at[g], recv_sem=srecv.at[z], device_id={"owner": s},
            ),
        )

    def back_arrive(p, first, owners):
        for ref, sem, each in ((recvb, brecv, short), (recvs, srecv, 1)):
            cut = pl.ds(first * each, owners * each)
            pltpu.make_async_remote_copy(
                src_ref=ref.at[:, cut], dst_ref=ref.at[:, cut],
                send_sem=bsend.at[0], recv_sem=sem.at[p], device_id={"owner": c_dev},
            ).wait_recv()

    def compute(k):
        chips = chips_of(k)
        codes = jnp.concatenate(
            [join(ms[2 * chip, me // 2], ms[2 * chip + 1, me // 2]) for chip in chips], axis=1
        )
        cluster = codes >> q_bits
        block_of = lax.broadcasted_iota(jnp.int32, (1, wide), 1) // cap
        source = (codes & (per_device - 1)) + block_of * per_device
        pick = jnp.where(
            lax.broadcasted_iota(jnp.int32, (rows, wide), 0) == source, 1.0, 0.0
        ).astype(jnp.bfloat16)
        block = jnp.concatenate(
            [qs[pl.ds(2 * chip, 2)].reshape(2 * per_device, width) for chip in chips], axis=0
        )
        rows_v[...] = lax.dot_general(
            block, pick, (((0,), (0,)), ((), ())), preferred_element_type=jnp.float32
        ).astype(jnp.bfloat16)
        count_of = jnp.concatenate([cntb[...], cntb[...]], axis=1)

        def one_half(g, carry):
            @pl.when(k == 0)
            def _():
                pltpu.make_async_copy(pass_v.at[g], pass_v.at[g], pass_sem.at[g]).wait()

            direct = lax.dot_general(
                pass_v[g], rows_v[...], (((1,), (0,)), ((), ())), preferred_element_type=jnp.float32
            )
            total = direct[:half]
            for u in range(1, clusters):
                total = jnp.where(
                    jnp.broadcast_to(cluster, (half, wide)) == u, direct[u * half : (u + 1) * half], total
                )
            acc[...] = total
            mine = lax.broadcasted_iota(jnp.int32, (clusters, wide), 0) == cluster
            term = jnp.sum(jnp.where(mine, direct[clusters * half :], 0.0), axis=0, keepdims=True)
            live = jnp.sum(jnp.where(mine, count_of, 0.0), axis=0, keepdims=True).astype(jnp.int32)
            place = lax.broadcasted_iota(jnp.int32, (half, wide), 0) + g * half
            value = jnp.where(place < live, acc[...] + term, 0.0)
            top = jnp.maximum(jnp.max(jnp.abs(value), axis=0, keepdims=True), 1e-30)
            coded = jnp.round(value * (TOP / top)).astype(jnp.int32)
            unit = top * (1.0 / TOP)
            for b, chip in enumerate(chips):
                part = coded[:, b * LANES : (b + 1) * LANES]
                packed = (pltpu.roll(part, LANES - short, 1) << 16) | (part & 0xFFFF)
                turned = jnp.transpose(packed)
                lane_unit = jnp.broadcast_to(unit[:, b * LANES : (b + 1) * LANES], (8, LANES))
                other = pltpu.roll(lane_unit, cap, 1)
                for i in range(2):
                    sendb[g, pl.ds((2 * chip + i) * short, short)] = turned[i * cap : i * cap + short]
                    sends[g, 2 * chip + i] = jnp.where((lane_row < cap) == (i == 0), lane_unit, other)[0:1]
            for i in range(4):
                s = 2 * chips[i // 2] + i % 2

                @pl.when(s == me)
                def _():
                    recvb[g, pl.ds(me * short, short)] = sendb[g, pl.ds(me * short, short)]
                    recvs[g, me] = sends[g, me]

                @pl.when(s != me)
                def _():
                    for copy in back_pair(g, s):
                        copy.start()

            @pl.when(g == 0)
            def _():
                service(k, (0, 2))

            @pl.when((g == 0) == (k > 0))
            def _():
                service(k, (1,))

            @pl.when((g == 1) & (k == 0) & (near > 0))
            def _():
                for h in (0, 2, 1):
                    forward_y(planes - 1, h)

            return carry

        lax.fori_loop(0, 2, one_half, 0)

    for h in (0, 2, 1):
        forward_z(1, h)
        forward_plane(1, h)

        @pl.when(near > 0)
        def _():
            forward_z(planes - 1, h)
            forward_c(planes - 1, h)

        relay_y(0, h)

    count_copy = pltpu.make_async_copy(ms.at[:, tables], cnt_s, load_sem.at[0])

    def step(k, carry):
        for chip in chips_of(k):
            for h in range(3):
                arrive(2 * chip + (1 - c), h)

        @pl.when(k == planes - 1)
        def _():
            count_copy.start()

        compute(k)
        return carry

    lax.fori_loop(0, planes, step, 0)

    count_copy.wait()

    def one_owner(o, seen):
        for l in range(clusters):
            seen = jnp.where(probe_v[...] == o * clusters + l, cnt_s[o, 0, l], seen)
        return seen

    seen = lax.fori_loop(0, n, one_owner, jnp.zeros((probe_count, per_device), jnp.int32))
    vis_ref[...] = jnp.sum(seen.astype(jnp.float32), axis=0, keepdims=True).astype(jnp.int32)

    def collect(k, carry):
        p = collect_of(k)
        base = p * 4
        @pl.when(p == z)
        def _():
            back_arrive(p, base, 3)

        @pl.when(p != z)
        def _():
            back_arrive(p, base, 4)

        quarter = lax.broadcasted_iota(jnp.int32, (8, LANES), 1) // short
        columns = []
        for g in range(2):
            straight = [jnp.broadcast_to(recvs[g, base + i], (8, LANES)) for i in range(4)]
            shifted = [pltpu.roll(row, short, 1) for row in straight]
            held = recvb[g, pl.ds(base * short, LANES)]
            halves = []
            for high in range(2):
                unit = jnp.zeros((8, LANES), jnp.float32)
                for i in range(4):
                    unit = jnp.where(quarter == i, straight[i] if i % 2 == high else shifted[i], unit)
                units = jnp.transpose(jnp.broadcast_to(unit[0:1], (LANES, LANES)))
                number = held >> 16 if high else (held << 16) >> 16
                halves.append(number.astype(jnp.float32) * units)
            columns.append(jnp.concatenate(halves, axis=0))
        value = jnp.concatenate(columns, axis=1)
        upper_part = value.astype(jnp.bfloat16)
        lower_part = (value - upper_part.astype(jnp.float32)).astype(jnp.bfloat16)
        at = slots[...] >> code_bits
        lane = lax.broadcasted_iota(jnp.int32, (pairs, LANES), 1)
        lane = (lane // short + base) * cap + lane % short
        chosen = jnp.concatenate(
            [jnp.where(at == lane + b * short, 1.0, 0.0).astype(jnp.bfloat16) for b in range(2)], axis=1
        )
        part = jnp.dot(chosen, upper_part, preferred_element_type=jnp.float32) + jnp.dot(
            chosen, lower_part, preferred_element_type=jnp.float32
        )

        @pl.when(k == 0)
        def _():
            out_ref[...] = part

        @pl.when(k > 0)
        def _():
            out_ref[...] += part

        return carry

    lax.fori_loop(0, planes, collect, 0)

    @pl.when(near > 0)
    def _():
        drain(0, planes + 1)

    @pl.when(near == 0)
    def _():
        drain(0, 1)

    drain(1, planes)
    drain(2, 2 * planes)
    for g in range(2):
        for ref, sem, each in ((sendb, bsend, short), (sends, ssend, 1)):
            cut = ref.at[g, pl.ds(0, (n - 1) * each)]
            pltpu.make_async_remote_copy(
                src_ref=cut, dst_ref=cut, send_sem=sem.at[g], recv_sem=brecv.at[0],
                device_id={"owner": c_dev},
            ).wait_send()


def fused_body(queries, probes, passages, centroids, counts):
    n = lax.axis_size("owner")
    per_device, probe_count = probes.shape
    clusters, span, width = passages.shape
    cap = 2 * per_device * probe_count // n
    pairs = per_device * probe_count
    tables = n * cap // LANES
    wide = 4 * cap
    vmem = pl.BlockSpec(memory_space=pltpu.VMEM)
    hbm = pl.BlockSpec(memory_space=pltpu.HBM)
    dma = pltpu.SemaphoreType.DMA
    scores, visits = pl.pallas_call(
        lambda *refs: owner_kernel(n, *refs),
        out_shape=(
            jax.ShapeDtypeStruct((pairs, span), jnp.float32),
            jax.ShapeDtypeStruct((1, per_device), jnp.int32),
        ),
        in_specs=[hbm] * 5,
        out_specs=(vmem, vmem),
        scratch_shapes=[
            pltpu.VMEM((2, clusters * span // 2 + clusters, width), jnp.bfloat16),
            pltpu.VMEM((n, per_device, width), jnp.bfloat16),
            pltpu.VMEM((1, clusters), jnp.int32),
            pltpu.VMEM((probe_count, per_device), jnp.int32),
            pltpu.VMEM((n, tables + 1, 1, LANES), jnp.int32),
            pltpu.VMEM((pairs, LANES), jnp.int32),
            pltpu.VMEM((width, wide), jnp.bfloat16),
            pltpu.VMEM((span // 2, wide), jnp.float32),
            pltpu.VMEM((clusters, LANES), jnp.float32),
            pltpu.VMEM((2, n * cap // 2, LANES), jnp.int32),
            pltpu.VMEM((2, n, 1, LANES), jnp.float32),
            pltpu.VMEM((2, n * cap // 2, LANES), jnp.int32),
            pltpu.VMEM((2, n, 1, LANES), jnp.float32),
            pltpu.SMEM((n, 1, LANES), jnp.int32),
            dma((2,)),
            dma((3,)),
            dma((3,)),
            dma((3,)),
            dma((n, 2)),
            dma((n,)),
            dma((2,)),
            dma((2,)),
            dma((n // 4,)),
            dma((n // 4,)),
        ],
        compiler_params=pltpu.CompilerParams(
            collective_id=0, has_side_effects=True, vmem_limit_bytes=48 * 2**20
        ),
    )(*[pltpu.with_memory_space_constraint(v, pltpu.HBM) for v in (queries, probes.T, passages, centroids, counts.reshape(1, clusters))])
    return scores.reshape(per_device, probe_count, span), visits.reshape(per_device)


def power_of_two(value):
    return value > 0 and value & (value - 1) == 0


def body(queries, probes, passages, centroids, counts):
    n = lax.axis_size("owner")
    per_device, probe_count = probes.shape
    clusters, span, width = passages.shape
    cap = 2 * per_device * probe_count // n
    held = 2 * width * (clusters * span + n * per_device)
    fits = (
        n == 16 and clusters % 16 == 0 and 2 * cap == LANES and n * probe_count == LANES and span == 2 * LANES
        and power_of_two(clusters) and power_of_two(per_device) and power_of_two(probe_count)
        and clusters <= LANES and per_device == cap
        and clusters * per_device * n * cap < 2**23 and width % LANES == 0 and held < 32 * 2**20
    )
    chosen = fused_body if fits else routed_body
    return chosen(queries, probes, passages, centroids, counts)


def solution(mesh):
    in_specs = (
        P(("groups", "owner"), None),
        P(("groups", "owner"), None),
        P("owner", None, None),
        P("owner", None),
        P("owner"),
    )
    out_specs = (P(("groups", "owner"), None, None), P(("groups", "owner")))
    return jax.shard_map(body, mesh=mesh, in_specs=in_specs, out_specs=out_specs, check_vma=False)
```

```python
import jax
import jax.numpy as jnp
from jax import lax
from jax.experimental import pallas as pl
from jax.experimental.pallas import tpu as pltpu
from jax.sharding import PartitionSpec as P


def routed_body(queries, probes, passages, centroids, counts):
    owner_count = lax.axis_size("owner")
    per_device, probe_count = probes.shape
    local_count, block_span, feature_width = passages.shape
    capacity = 2 * per_device * probe_count // owner_count
    pair_count = per_device * probe_count
    passage_blocks = jnp.transpose(passages, (0, 2, 1))
    flat_probes = probes.reshape(-1)
    target_owner = flat_probes // local_count
    target_local = flat_probes % local_count
    owner_hits = (
        target_owner[:, None] == jnp.arange(owner_count, dtype=jnp.int32)[None, :]
    ).astype(jnp.int32)
    slot_rank = jnp.sum((jnp.cumsum(owner_hits, axis=0) - owner_hits) * owner_hits, axis=1)
    slot_index = target_owner * capacity + slot_rank
    pair_ids = jnp.arange(pair_count, dtype=jnp.int32)
    slot_match = slot_index[None, :] == jnp.arange(owner_count * capacity, dtype=jnp.int32)[:, None]
    slot_filled = jnp.any(slot_match, axis=1)
    source_pair = jnp.sum(jnp.where(slot_match, pair_ids[None, :], 0), axis=1)
    send_rows = jnp.where(
        slot_filled[:, None], queries[source_pair // probe_count], jnp.zeros((), jnp.bfloat16)
    )
    send_ids = jnp.where(slot_filled, target_local[source_pair], -1)
    query_rows = lax.all_to_all(
        send_rows.reshape(owner_count, capacity, feature_width),
        "owner",
        split_axis=0,
        concat_axis=0,
        tiled=True,
    )
    cluster_ids = lax.all_to_all(
        send_ids.reshape(owner_count, capacity), "owner", split_axis=0, concat_axis=0, tiled=True
    )
    source_count, slot_count = cluster_ids.shape
    row_total = source_count * slot_count
    flat_rows = query_rows.reshape(row_total, feature_width)
    flat_ids = cluster_ids.reshape(-1)
    group_ids = jnp.where(flat_ids < 0, 0, flat_ids).astype(jnp.int32)
    cluster_pick = flat_ids[:, None] == jnp.arange(local_count, dtype=jnp.int32)[None, :]
    live_sizes = jnp.sum(jnp.where(cluster_pick, counts[None, :], 0), axis=1)
    group_pick = group_ids[:, None] == jnp.arange(local_count, dtype=jnp.int32)[None, :]
    group_sizes = jnp.sum(group_pick.astype(jnp.int32), axis=0)
    order = jnp.argsort(group_ids, stable=True)
    undo_order = jnp.argsort(order, stable=True)
    sorted_rows = flat_rows[order]
    sorted_scores = lax.ragged_dot(
        sorted_rows, passage_blocks, group_sizes, preferred_element_type=jnp.float32
    )
    own_scores = sorted_scores[undo_order]
    centre_term = jnp.einsum(
        "rd,rd->r", flat_rows, centroids[group_ids], preferred_element_type=jnp.float32
    )
    live_mask = jnp.arange(block_span, dtype=jnp.int32)[None, :] < live_sizes[:, None]
    masked_scores = jnp.where(live_mask, own_scores + centre_term[:, None], 0.0)
    back_scores = lax.all_to_all(
        masked_scores.reshape(source_count, slot_count, block_span),
        "owner",
        split_axis=0,
        concat_axis=0,
        tiled=True,
    )
    back_sizes = lax.all_to_all(
        live_sizes.astype(jnp.float32).reshape(source_count, slot_count),
        "owner",
        split_axis=0,
        concat_axis=0,
        tiled=True,
    )
    flat_scores = back_scores.reshape(owner_count * capacity, block_span)
    scores = flat_scores[slot_index].reshape(per_device, probe_count, block_span)
    pair_sizes = back_sizes.reshape(-1)[slot_index].reshape(per_device, probe_count)
    visits = jnp.sum(pair_sizes, axis=1).astype(jnp.int32)
    return (scores, visits)


LANES = 128
TOP = 32767.0


def owner_kernel(
    n, q_hbm, probe_hbm, pass_hbm, cent_hbm, cnt_hbm,
    out_ref, vis_ref,
    pass_v, qs, cnt_v, probe_v, ms, slots, rows_v, acc, cntb, sendb, sends, recvb, recvs, cnt_s,
    pass_sem, load_sem, qsend, msend, qrecv, mrecv, bsend, ssend, brecv, srecv,
):
    clusters, width = cent_hbm.shape
    span = pass_hbm.shape[1]
    probe_count, per_device = probe_v.shape
    pairs = probe_count * per_device
    planes = n // 4
    rows = 4 * per_device
    tables = ms.shape[1] - 1
    cap = LANES // 2
    wide = 4 * cap
    half = span // 2
    short = cap // 2
    piece = per_device // 2
    code_bits = (clusters * per_device).bit_length() - 1
    q_bits = per_device.bit_length() - 1
    cl_bits = clusters.bit_length() - 1
    me = lax.axis_index("owner")
    z = me // 4
    y = (me // 2) % 2
    c = me % 2
    y_dev = z * 4 + (1 - y) * 2 + c
    c_dev = z * 4 + y * 2 + (1 - c)
    has_low = z > 0
    has_high = z < planes - 1

    loads = [
        pltpu.make_async_copy(q_hbm, qs.at[me], load_sem.at[0]),
        pltpu.make_async_copy(probe_hbm, probe_v, load_sem.at[1]),
        pltpu.make_async_copy(cnt_hbm, cnt_v, load_sem.at[2]),
    ]
    for copy in loads:
        copy.start()

    barrier = pltpu.get_barrier_semaphore()

    def greet(dev):
        pl.semaphore_signal(barrier, inc=1, device_id={"owner": dev})

    greet(y_dev)
    greet(c_dev)

    @pl.when(has_low)
    def _():
        greet(me - 4)

    @pl.when(has_high)
    def _():
        greet(me + 4)

    def passage_copies(g):
        return [
            pltpu.make_async_copy(
                pass_hbm.at[k, pl.ds(g * half, half)], pass_v.at[g, pl.ds(k * half, half)], pass_sem.at[g]
            )
            for k in range(clusters)
        ] + [
            pltpu.make_async_copy(cent_hbm, pass_v.at[g, pl.ds(clusters * half, clusters)], pass_sem.at[g])
        ]

    for g in range(2):
        for copy in passage_copies(g):
            copy.start()

    loads[0].wait()
    pl.semaphore_wait(barrier, 2 + jnp.where(has_low, 1, 0) + jnp.where(has_high, 1, 0))

    def chunk(s, h, target, dev):
        if h == 2:
            return pltpu.make_async_remote_copy(
                src_ref=ms.at[s], dst_ref=ms.at[s],
                send_sem=msend.at[max(target - 1, 0)], recv_sem=mrecv.at[s], device_id={"owner": dev},
            )
        cut = pl.ds(h * piece, piece)
        return pltpu.make_async_remote_copy(
            src_ref=qs.at[s, cut], dst_ref=qs.at[s, cut],
            send_sem=qsend.at[max(target - 1, 0)], recv_sem=qrecv.at[s, h], device_id={"owner": dev},
        )

    def push(s, h, target, dev):
        chunk(s, h, target, dev).start()

    def drain(way, blocks):
        for ref, sem in ((qs, qsend), (ms, msend)):
            pltpu.make_async_remote_copy(
                src_ref=ref.at[pl.ds(0, blocks)], dst_ref=ref.at[pl.ds(0, blocks)],
                send_sem=sem.at[way], recv_sem=mrecv.at[0], device_id={"owner": c_dev},
            ).wait_send()

    def arrive(s, h):
        chunk(s, h, 0, c_dev).wait_recv()

    def onward(act, s, h, low, high):
        @pl.when(low)
        def _():
            act(s, h, 0, me - 4)

        @pl.when(high)
        def _():
            act(s, h, 1, me + 4)

        act(s, h, 2, y_dev)
        act(s, h, 3, c_dev)

    onward(push, me, 0, has_low, has_high)

    for copy in loads[1:]:
        copy.wait()

    def lower(row):
        return jnp.where(c == 1, pltpu.roll(row, cap, 1), row)

    def upper(row):
        return jnp.where(c == 1, row, pltpu.roll(row, cap, 1))

    lane_row = lax.broadcasted_iota(jnp.int32, (8, LANES), 1)

    def join(first, second):
        first = jnp.broadcast_to(first, (8, LANES))
        second = jnp.broadcast_to(second, (8, LANES))
        return jnp.where(lane_row < cap, lower(first), upper(second))[0:1]

    probes = probe_v[...]
    target = probes >> cl_bits
    local = probes & (clusters - 1)
    hits = jnp.concatenate(
        [jnp.where(target == o, 1.0, 0.0).astype(jnp.float32) for o in range(n)], axis=0
    ).astype(jnp.bfloat16)
    big = n * probe_count
    r_iota = lax.broadcasted_iota(jnp.int32, (big, big), 0)
    c_iota = lax.broadcasted_iota(jnp.int32, (big, big), 1)
    p_bits = probe_count.bit_length() - 1
    earlier = jnp.where(
        ((r_iota >> p_bits) == (c_iota >> p_bits)) & (c_iota < r_iota), 1.0, 0.0
    ).astype(jnp.bfloat16)
    before = jnp.where(
        lax.broadcasted_iota(jnp.int32, (per_device, per_device), 0)
        < lax.broadcasted_iota(jnp.int32, (per_device, per_device), 1), 1.0, 0.0,
    ).astype(jnp.bfloat16)
    lead = jnp.dot(earlier, hits, preferred_element_type=jnp.float32).astype(jnp.bfloat16)
    ranks = jnp.dot(hits, before, preferred_element_type=jnp.float32) + jnp.dot(
        lead, jnp.ones((per_device, per_device), jnp.bfloat16), preferred_element_type=jnp.float32
    )
    rank = jnp.zeros((probe_count, per_device), jnp.float32)
    for o in range(n):
        rank = jnp.where(target == o, ranks[o * probe_count : (o + 1) * probe_count], rank)
    slot = target * cap + rank.astype(jnp.int32)
    code = local * per_device + lax.broadcasted_iota(jnp.int32, (probe_count, per_device), 1)
    word = (slot << code_bits) | code
    for q in range(per_device):
        slots[q * probe_count : (q + 1) * probe_count, :] = jnp.broadcast_to(
            word[:, q : q + 1], (probe_count, LANES)
        )

    def one_table(b, carry):
        lane = lax.broadcasted_iota(jnp.int32, (pairs, LANES), 1) + b * LANES
        held = slots[...]
        found = jnp.where((held >> code_bits) == lane, held & ((1 << code_bits) - 1), 0)
        ms[me, b] = jnp.sum(found.astype(jnp.float32), axis=0, keepdims=True).astype(jnp.int32)
        return carry

    lax.fori_loop(0, tables, one_table, 0)
    ms[me, tables] = jnp.zeros((1, LANES), jnp.int32)
    ms[me, tables, :, 0:clusters] = cnt_v[...]
    onward(push, me, 2, has_low, has_high)
    onward(push, me, 1, has_low, has_high)
    live_row = ms[me, tables].astype(jnp.float32)
    cntb[...] = jnp.transpose(jnp.broadcast_to(live_row, (LANES, LANES)))[0:clusters]

    near = jnp.minimum(z, planes - 1 - z)
    long_side = jnp.where(z < planes - 1 - z, 1, -1)

    far = planes - 1 - near

    def plane_of(k):
        return z + long_side * jnp.where(k <= far, k, far - k)

    def collect_of(k):
        ends = jnp.where(k == 1, 2, jnp.where(k == 2, 1, k))
        inner = jnp.where(k == 1, -1, jnp.where(k > 1, k - 1, 0))
        return z + long_side * jnp.where(near == 0, ends, inner)

    def pick_of(u, values):
        found = values[0]
        for at in range(1, len(values)):
            found = jnp.where(u == at, values[at], found)
        return found

    def chips_of(u):
        inner = near > 0
        first = pick_of(u, (1, 2, jnp.where(inner, 2, 3), 3))
        first_far = pick_of(u, (0, 0, jnp.where(inner, 1, 0), jnp.where(inner, 0, 1)))
        second = pick_of(u, (0, jnp.where(inner, 1, 0), jnp.where(inner, 0, 1), jnp.where(inner, 3, 2)))
        second_far = pick_of(u, (0, 1, 1, 1))

        def chip(k, other):
            return plane_of(k) * 2 + jnp.where(other == 1, 1 - y, y)

        return chip(first, first_far), chip(second, second_far)

    def along(k):
        return plane_of(k) * 4 + y * 2 + c

    def forward_z(k, h, act=push, wait=True):
        p = plane_of(k)
        if wait:
            arrive(along(k), h)

        @pl.when((p > z) & has_low)
        def _():
            act(along(k), h, 0, me - 4)

        @pl.when((p < z) & has_high)
        def _():
            act(along(k), h, 1, me + 4)

    def forward_y(k, h, act=push):
        act(along(k), h, 2, y_dev)

    def forward_c(k, h, act=push):
        act(along(k), h, 3, c_dev)

    def forward_plane(k, h, act=push):
        forward_y(k, h, act)
        forward_c(k, h, act)

    def relay_y(k, h):
        s = plane_of(k) * 4 + (1 - y) * 2 + c
        arrive(s, h)
        push(s, h, 3, c_dev)

    def service(u, pieces):
        for h in pieces:
            @pl.when(u + 2 <= far)
            def _():
                forward_z(u + 2, h)
                forward_plane(u + 2, h)

            @pl.when(u + 1 < planes)
            def _():
                relay_y(u + 1, h)

    def back_pair(g, s):
        return (
            pltpu.make_async_remote_copy(
                src_ref=sendb.at[g, pl.ds(s * short, short)],
                dst_ref=recvb.at[g, pl.ds(me * short, short)],
                send_sem=bsend.at[g], recv_sem=brecv.at[z], device_id={"owner": s},
            ),
            pltpu.make_async_remote_copy(
                src_ref=sends.at[g, s], dst_ref=recvs.at[g, me],
                send_sem=ssend.at[g], recv_sem=srecv.at[z], device_id={"owner": s},
            ),
        )

    def back_arrive(p, first, owners):
        for ref, sem, each in ((recvb, brecv, short), (recvs, srecv, 1)):
            cut = pl.ds(first * each, owners * each)
            pltpu.make_async_remote_copy(
                src_ref=ref.at[:, cut], dst_ref=ref.at[:, cut],
                send_sem=bsend.at[0], recv_sem=sem.at[p], device_id={"owner": c_dev},
            ).wait_recv()

    def compute(k):
        chips = chips_of(k)
        codes = jnp.concatenate(
            [join(ms[2 * chip, me // 2], ms[2 * chip + 1, me // 2]) for chip in chips], axis=1
        )
        cluster = codes >> q_bits
        block_of = lax.broadcasted_iota(jnp.int32, (1, wide), 1) // cap
        source = (codes & (per_device - 1)) + block_of * per_device
        pick = jnp.where(
            lax.broadcasted_iota(jnp.int32, (rows, wide), 0) == source, 1.0, 0.0
        ).astype(jnp.bfloat16)
        block = jnp.concatenate(
            [qs[pl.ds(2 * chip, 2)].reshape(2 * per_device, width) for chip in chips], axis=0
        )
        rows_v[...] = lax.dot_general(
            block, pick, (((0,), (0,)), ((), ())), preferred_element_type=jnp.float32
        ).astype(jnp.bfloat16)
        count_of = jnp.concatenate([cntb[...], cntb[...]], axis=1)

        def one_half(g, carry):
            @pl.when(k == 0)
            def _():
                pltpu.make_async_copy(pass_v.at[g], pass_v.at[g], pass_sem.at[g]).wait()

            direct = lax.dot_general(
                pass_v[g], rows_v[...], (((1,), (0,)), ((), ())), preferred_element_type=jnp.float32
            )
            total = direct[:half]
            for u in range(1, clusters):
                total = jnp.where(
                    jnp.broadcast_to(cluster, (half, wide)) == u, direct[u * half : (u + 1) * half], total
                )
            acc[...] = total
            mine = lax.broadcasted_iota(jnp.int32, (clusters, wide), 0) == cluster
            term = jnp.sum(jnp.where(mine, direct[clusters * half :], 0.0), axis=0, keepdims=True)
            live = jnp.sum(jnp.where(mine, count_of, 0.0), axis=0, keepdims=True).astype(jnp.int32)
            place = lax.broadcasted_iota(jnp.int32, (half, wide), 0) + g * half
            value = jnp.where(place < live, acc[...] + term, 0.0)
            top = jnp.maximum(jnp.max(jnp.abs(value), axis=0, keepdims=True), 1e-30)
            coded = jnp.round(value * (TOP / top)).astype(jnp.int32)
            unit = top * (1.0 / TOP)
            for b, chip in enumerate(chips):
                part = coded[:, b * LANES : (b + 1) * LANES]
                packed = (pltpu.roll(part, LANES - short, 1) << 16) | (part & 0xFFFF)
                turned = jnp.transpose(packed)
                lane_unit = jnp.broadcast_to(unit[:, b * LANES : (b + 1) * LANES], (8, LANES))
                other = pltpu.roll(lane_unit, cap, 1)
                for i in range(2):
                    sendb[g, pl.ds((2 * chip + i) * short, short)] = turned[i * cap : i * cap + short]
                    sends[g, 2 * chip + i] = jnp.where((lane_row < cap) == (i == 0), lane_unit, other)[0:1]
            for i in range(4):
                s = 2 * chips[i // 2] + i % 2

                @pl.when(s == me)
                def _():
                    recvb[g, pl.ds(me * short, short)] = sendb[g, pl.ds(me * short, short)]
                    recvs[g, me] = sends[g, me]

                @pl.when(s != me)
                def _():
                    for copy in back_pair(g, s):
                        copy.start()

            @pl.when(g == 0)
            def _():
                service(k, (0, 2))

            @pl.when(g == 0)
            def _():
                service(k, (1,))

            return carry

        lax.fori_loop(0, 2, one_half, 0)

    for h in (0, 2, 1):
        forward_z(1, h)
        forward_plane(1, h)

        @pl.when(near > 0)
        def _():
            forward_z(planes - 1, h)
            forward_plane(planes - 1, h)

        relay_y(0, h)

    count_copy = pltpu.make_async_copy(ms.at[:, tables], cnt_s, load_sem.at[0])

    def step(k, carry):
        for chip in chips_of(k):
            for h in range(3):
                arrive(2 * chip + (1 - c), h)

        @pl.when(k == planes - 1)
        def _():
            count_copy.start()

        compute(k)
        return carry

    lax.fori_loop(0, planes, step, 0)

    count_copy.wait()

    def one_owner(o, seen):
        for l in range(clusters):
            seen = jnp.where(probe_v[...] == o * clusters + l, cnt_s[o, 0, l], seen)
        return seen

    seen = lax.fori_loop(0, n, one_owner, jnp.zeros((probe_count, per_device), jnp.int32))
    vis_ref[...] = jnp.sum(seen.astype(jnp.float32), axis=0, keepdims=True).astype(jnp.int32)

    def collect(k, carry):
        p = collect_of(k)
        base = p * 4
        @pl.when(p == z)
        def _():
            back_arrive(p, base, 3)

        @pl.when(p != z)
        def _():
            back_arrive(p, base, 4)

        quarter = lax.broadcasted_iota(jnp.int32, (8, LANES), 1) // short
        columns = []
        for g in range(2):
            straight = [jnp.broadcast_to(recvs[g, base + i], (8, LANES)) for i in range(4)]
            shifted = [pltpu.roll(row, short, 1) for row in straight]
            held = recvb[g, pl.ds(base * short, LANES)]
            halves = []
            for high in range(2):
                unit = jnp.zeros((8, LANES), jnp.float32)
                for i in range(4):
                    unit = jnp.where(quarter == i, straight[i] if i % 2 == high else shifted[i], unit)
                units = jnp.transpose(jnp.broadcast_to(unit[0:1], (LANES, LANES)))
                number = held >> 16 if high else (held << 16) >> 16
                halves.append(number.astype(jnp.float32) * units)
            columns.append(jnp.concatenate(halves, axis=0))
        value = jnp.concatenate(columns, axis=1)
        upper_part = value.astype(jnp.bfloat16)
        lower_part = (value - upper_part.astype(jnp.float32)).astype(jnp.bfloat16)
        at = slots[...] >> code_bits
        lane = lax.broadcasted_iota(jnp.int32, (pairs, LANES), 1)
        lane = (lane // short + base) * cap + lane % short
        chosen = jnp.concatenate(
            [jnp.where(at == lane + b * short, 1.0, 0.0).astype(jnp.bfloat16) for b in range(2)], axis=1
        )
        part = jnp.dot(chosen, upper_part, preferred_element_type=jnp.float32) + jnp.dot(
            chosen, lower_part, preferred_element_type=jnp.float32
        )

        @pl.when(k == 0)
        def _():
            out_ref[...] = part

        @pl.when(k > 0)
        def _():
            out_ref[...] += part

        return carry

    lax.fori_loop(0, planes, collect, 0)

    @pl.when(near > 0)
    def _():
        drain(0, planes + 1)

    @pl.when(near == 0)
    def _():
        drain(0, 1)

    drain(1, planes)
    drain(2, 2 * planes)
    for g in range(2):
        for ref, sem, each in ((sendb, bsend, short), (sends, ssend, 1)):
            cut = ref.at[g, pl.ds(0, (n - 1) * each)]
            pltpu.make_async_remote_copy(
                src_ref=cut, dst_ref=cut, send_sem=sem.at[g], recv_sem=brecv.at[0],
                device_id={"owner": c_dev},
            ).wait_send()


def deliver(scores_ref, visits_ref, scores_out, visits_out, sem):
    copies = (
        pltpu.make_async_copy(scores_ref, scores_out, sem.at[0]),
        pltpu.make_async_copy(visits_ref, visits_out, sem.at[1]),
    )
    for copy in copies:
        copy.start()
    for copy in copies:
        copy.wait()


def fused_body(queries, probes, passages, centroids, counts):
    n = lax.axis_size("owner")
    per_device, probe_count = probes.shape
    clusters, span, width = passages.shape
    cap = 2 * per_device * probe_count // n
    pairs = per_device * probe_count
    tables = n * cap // LANES
    wide = 4 * cap
    vmem = pl.BlockSpec(memory_space=pltpu.VMEM)
    hbm = pl.BlockSpec(memory_space=pltpu.HBM)
    dma = pltpu.SemaphoreType.DMA
    scores, visits = pl.pallas_call(
        lambda *refs: owner_kernel(n, *refs),
        out_shape=(
            jax.ShapeDtypeStruct((pairs, span), jnp.float32),
            jax.ShapeDtypeStruct((1, per_device), jnp.int32),
        ),
        in_specs=[hbm] * 5,
        out_specs=(vmem, vmem),
        scratch_shapes=[
            pltpu.VMEM((2, clusters * span // 2 + clusters, width), jnp.bfloat16),
            pltpu.VMEM((n, per_device, width), jnp.bfloat16),
            pltpu.VMEM((1, clusters), jnp.int32),
            pltpu.VMEM((probe_count, per_device), jnp.int32),
            pltpu.VMEM((n, tables + 1, 1, LANES), jnp.int32),
            pltpu.VMEM((pairs, LANES), jnp.int32),
            pltpu.VMEM((width, wide), jnp.bfloat16),
            pltpu.VMEM((span // 2, wide), jnp.float32),
            pltpu.VMEM((clusters, LANES), jnp.float32),
            pltpu.VMEM((2, n * cap // 2, LANES), jnp.int32),
            pltpu.VMEM((2, n, 1, LANES), jnp.float32),
            pltpu.VMEM((2, n * cap // 2, LANES), jnp.int32),
            pltpu.VMEM((2, n, 1, LANES), jnp.float32),
            pltpu.SMEM((n, 1, LANES), jnp.int32),
            dma((2,)),
            dma((3,)),
            dma((3,)),
            dma((3,)),
            dma((n, 2)),
            dma((n,)),
            dma((2,)),
            dma((2,)),
            dma((n // 4,)),
            dma((n // 4,)),
        ],
        compiler_params=pltpu.CompilerParams(
            collective_id=0, has_side_effects=True, vmem_limit_bytes=48 * 2**20
        ),
    )(*[pltpu.with_memory_space_constraint(v, pltpu.HBM) for v in (queries, probes.T, passages, centroids, counts.reshape(1, clusters))])
    scores, visits = pl.pallas_call(
        deliver,
        out_shape=(
            jax.ShapeDtypeStruct((pairs, span), jnp.float32),
            jax.ShapeDtypeStruct((1, per_device), jnp.int32),
        ),
        in_specs=[vmem] * 2,
        out_specs=(pl.BlockSpec(memory_space=pl.ANY), pl.BlockSpec(memory_space=pl.ANY)),
        scratch_shapes=[dma((2,))],
        compiler_params=pltpu.CompilerParams(vmem_limit_bytes=2**20),
    )(*[pltpu.with_memory_space_constraint(v, pltpu.VMEM) for v in (scores, visits)])
    return scores.reshape(per_device, probe_count, span), visits.reshape(per_device)


def power_of_two(value):
    return value > 0 and value & (value - 1) == 0


def body(queries, probes, passages, centroids, counts):
    n = lax.axis_size("owner")
    per_device, probe_count = probes.shape
    clusters, span, width = passages.shape
    cap = 2 * per_device * probe_count // n
    held = 2 * width * (clusters * span + n * per_device)
    fits = (
        n == 16 and clusters % 16 == 0 and 2 * cap == LANES and n * probe_count == LANES and span == 2 * LANES
        and power_of_two(clusters) and power_of_two(per_device) and power_of_two(probe_count)
        and clusters <= LANES and per_device == cap
        and clusters * per_device * n * cap < 2**23 and width % LANES == 0 and held < 32 * 2**20
    )
    chosen = fused_body if fits else routed_body
    return chosen(queries, probes, passages, centroids, counts)


def solution(mesh):
    in_specs = (
        P(("groups", "owner"), None),
        P(("groups", "owner"), None),
        P("owner", None, None),
        P("owner", None),
        P("owner"),
    )
    out_specs = (P(("groups", "owner"), None, None), P(("groups", "owner")))
    return jax.shard_map(body, mesh=mesh, in_specs=in_specs, out_specs=out_specs, check_vma=False)
```

```python
import jax
import jax.numpy as jnp
from jax import lax
from jax.experimental import pallas as pl
from jax.experimental.pallas import tpu as pltpu
from jax.sharding import PartitionSpec as P


def routed_body(queries, probes, passages, centroids, counts):
    owner_count = lax.axis_size("owner")
    per_device, probe_count = probes.shape
    local_count, block_span, feature_width = passages.shape
    capacity = 2 * per_device * probe_count // owner_count
    pair_count = per_device * probe_count
    passage_blocks = jnp.transpose(passages, (0, 2, 1))
    flat_probes = probes.reshape(-1)
    target_owner = flat_probes // local_count
    target_local = flat_probes % local_count
    owner_hits = (
        target_owner[:, None] == jnp.arange(owner_count, dtype=jnp.int32)[None, :]
    ).astype(jnp.int32)
    slot_rank = jnp.sum((jnp.cumsum(owner_hits, axis=0) - owner_hits) * owner_hits, axis=1)
    slot_index = target_owner * capacity + slot_rank
    pair_ids = jnp.arange(pair_count, dtype=jnp.int32)
    slot_match = slot_index[None, :] == jnp.arange(owner_count * capacity, dtype=jnp.int32)[:, None]
    slot_filled = jnp.any(slot_match, axis=1)
    source_pair = jnp.sum(jnp.where(slot_match, pair_ids[None, :], 0), axis=1)
    send_rows = jnp.where(
        slot_filled[:, None], queries[source_pair // probe_count], jnp.zeros((), jnp.bfloat16)
    )
    send_ids = jnp.where(slot_filled, target_local[source_pair], -1)
    query_rows = lax.all_to_all(
        send_rows.reshape(owner_count, capacity, feature_width),
        "owner",
        split_axis=0,
        concat_axis=0,
        tiled=True,
    )
    cluster_ids = lax.all_to_all(
        send_ids.reshape(owner_count, capacity), "owner", split_axis=0, concat_axis=0, tiled=True
    )
    source_count, slot_count = cluster_ids.shape
    row_total = source_count * slot_count
    flat_rows = query_rows.reshape(row_total, feature_width)
    flat_ids = cluster_ids.reshape(-1)
    group_ids = jnp.where(flat_ids < 0, 0, flat_ids).astype(jnp.int32)
    cluster_pick = flat_ids[:, None] == jnp.arange(local_count, dtype=jnp.int32)[None, :]
    live_sizes = jnp.sum(jnp.where(cluster_pick, counts[None, :], 0), axis=1)
    group_pick = group_ids[:, None] == jnp.arange(local_count, dtype=jnp.int32)[None, :]
    group_sizes = jnp.sum(group_pick.astype(jnp.int32), axis=0)
    order = jnp.argsort(group_ids, stable=True)
    undo_order = jnp.argsort(order, stable=True)
    sorted_rows = flat_rows[order]
    sorted_scores = lax.ragged_dot(
        sorted_rows, passage_blocks, group_sizes, preferred_element_type=jnp.float32
    )
    own_scores = sorted_scores[undo_order]
    centre_term = jnp.einsum(
        "rd,rd->r", flat_rows, centroids[group_ids], preferred_element_type=jnp.float32
    )
    live_mask = jnp.arange(block_span, dtype=jnp.int32)[None, :] < live_sizes[:, None]
    masked_scores = jnp.where(live_mask, own_scores + centre_term[:, None], 0.0)
    back_scores = lax.all_to_all(
        masked_scores.reshape(source_count, slot_count, block_span),
        "owner",
        split_axis=0,
        concat_axis=0,
        tiled=True,
    )
    back_sizes = lax.all_to_all(
        live_sizes.astype(jnp.float32).reshape(source_count, slot_count),
        "owner",
        split_axis=0,
        concat_axis=0,
        tiled=True,
    )
    flat_scores = back_scores.reshape(owner_count * capacity, block_span)
    scores = flat_scores[slot_index].reshape(per_device, probe_count, block_span)
    pair_sizes = back_sizes.reshape(-1)[slot_index].reshape(per_device, probe_count)
    visits = jnp.sum(pair_sizes, axis=1).astype(jnp.int32)
    return (scores, visits)


LANES = 128
TOP = 32767.0


def owner_kernel(
    n, q_hbm, probe_hbm, pass_hbm, cent_hbm, cnt_hbm,
    out_ref, vis_ref,
    pass_v, qs, cnt_v, probe_v, ms, slots, rows_v, acc, cntb, sendb, sends, recvb, recvs, cnt_s,
    pass_sem, load_sem, qsend, msend, qrecv, mrecv, bsend, ssend, brecv, srecv,
):
    clusters, width = cent_hbm.shape
    span = pass_hbm.shape[1]
    probe_count, per_device = probe_v.shape
    pairs = probe_count * per_device
    planes = n // 4
    rows = 4 * per_device
    tables = ms.shape[1] - 1
    cap = LANES // 2
    wide = 4 * cap
    half = span // 2
    short = cap // 2
    piece = per_device // 2
    code_bits = (clusters * per_device).bit_length() - 1
    q_bits = per_device.bit_length() - 1
    cl_bits = clusters.bit_length() - 1
    me = lax.axis_index("owner")
    z = me // 4
    y = (me // 2) % 2
    c = me % 2
    y_dev = z * 4 + (1 - y) * 2 + c
    c_dev = z * 4 + y * 2 + (1 - c)
    has_low = z > 0
    has_high = z < planes - 1

    loads = [
        pltpu.make_async_copy(q_hbm, qs.at[me], load_sem.at[0]),
        pltpu.make_async_copy(probe_hbm, probe_v, load_sem.at[1]),
        pltpu.make_async_copy(cnt_hbm, cnt_v, load_sem.at[2]),
    ]
    for copy in loads:
        copy.start()

    barrier = pltpu.get_barrier_semaphore()

    def greet(dev):
        pl.semaphore_signal(barrier, inc=1, device_id={"owner": dev})

    greet(y_dev)
    greet(c_dev)

    @pl.when(has_low)
    def _():
        greet(me - 4)

    @pl.when(has_high)
    def _():
        greet(me + 4)

    def passage_copies(g):
        return [
            pltpu.make_async_copy(
                pass_hbm.at[k, pl.ds(g * half, half)], pass_v.at[g, pl.ds(k * half, half)], pass_sem.at[g]
            )
            for k in range(clusters)
        ] + [
            pltpu.make_async_copy(cent_hbm, pass_v.at[g, pl.ds(clusters * half, clusters)], pass_sem.at[g])
        ]

    for g in range(2):
        for copy in passage_copies(g):
            copy.start()

    loads[0].wait()
    pl.semaphore_wait(barrier, 2 + jnp.where(has_low, 1, 0) + jnp.where(has_high, 1, 0))

    def chunk(s, h, target, dev):
        if h == 2:
            return pltpu.make_async_remote_copy(
                src_ref=ms.at[s], dst_ref=ms.at[s],
                send_sem=msend.at[max(target - 1, 0)], recv_sem=mrecv.at[s], device_id={"owner": dev},
            )
        cut = pl.ds(h * piece, piece)
        return pltpu.make_async_remote_copy(
            src_ref=qs.at[s, cut], dst_ref=qs.at[s, cut],
            send_sem=qsend.at[max(target - 1, 0)], recv_sem=qrecv.at[s, h], device_id={"owner": dev},
        )

    def push(s, h, target, dev):
        chunk(s, h, target, dev).start()

    def drain(way, blocks, halves):
        for cut, sem in (
            (pass_v.at[0, pl.ds(0, halves * piece)], qsend),
            (ms.at[pl.ds(0, blocks)], msend),
        ):
            pltpu.make_async_remote_copy(
                src_ref=cut, dst_ref=cut, send_sem=sem.at[way], recv_sem=mrecv.at[0],
                device_id={"owner": c_dev},
            ).wait_send()

    def arrive(s, h):
        chunk(s, h, 0, c_dev).wait_recv()

    def onward(act, s, h, low, high):
        @pl.when(low)
        def _():
            act(s, h, 0, me - 4)

        @pl.when(high)
        def _():
            act(s, h, 1, me + 4)

        act(s, h, 2, y_dev)
        act(s, h, 3, c_dev)

    onward(push, me, 0, has_low, has_high)

    for copy in loads[1:]:
        copy.wait()

    def lower(row):
        return jnp.where(c == 1, pltpu.roll(row, cap, 1), row)

    def upper(row):
        return jnp.where(c == 1, row, pltpu.roll(row, cap, 1))

    lane_row = lax.broadcasted_iota(jnp.int32, (8, LANES), 1)

    def join(first, second):
        first = jnp.broadcast_to(first, (8, LANES))
        second = jnp.broadcast_to(second, (8, LANES))
        return jnp.where(lane_row < cap, lower(first), upper(second))[0:1]

    probes = probe_v[...]
    target = probes >> cl_bits
    local = probes & (clusters - 1)
    hits = jnp.concatenate(
        [jnp.where(target == o, 1.0, 0.0).astype(jnp.float32) for o in range(n)], axis=0
    ).astype(jnp.bfloat16)
    big = n * probe_count
    r_iota = lax.broadcasted_iota(jnp.int32, (big, big), 0)
    c_iota = lax.broadcasted_iota(jnp.int32, (big, big), 1)
    p_bits = probe_count.bit_length() - 1
    earlier = jnp.where(
        ((r_iota >> p_bits) == (c_iota >> p_bits)) & (c_iota < r_iota), 1.0, 0.0
    ).astype(jnp.bfloat16)
    before = jnp.where(
        lax.broadcasted_iota(jnp.int32, (per_device, per_device), 0)
        < lax.broadcasted_iota(jnp.int32, (per_device, per_device), 1), 1.0, 0.0,
    ).astype(jnp.bfloat16)
    lead = jnp.dot(earlier, hits, preferred_element_type=jnp.float32).astype(jnp.bfloat16)
    ranks = jnp.dot(hits, before, preferred_element_type=jnp.float32) + jnp.dot(
        lead, jnp.ones((per_device, per_device), jnp.bfloat16), preferred_element_type=jnp.float32
    )
    rank = jnp.zeros((probe_count, per_device), jnp.float32)
    for o in range(n):
        rank = jnp.where(target == o, ranks[o * probe_count : (o + 1) * probe_count], rank)
    slot = target * cap + rank.astype(jnp.int32)
    code = local * per_device + lax.broadcasted_iota(jnp.int32, (probe_count, per_device), 1)
    word = (slot << code_bits) | code
    for q in range(per_device):
        slots[q * probe_count : (q + 1) * probe_count, :] = jnp.broadcast_to(
            word[:, q : q + 1], (probe_count, LANES)
        )

    def one_table(b, carry):
        lane = lax.broadcasted_iota(jnp.int32, (pairs, LANES), 1) + b * LANES
        held = slots[...]
        found = jnp.where((held >> code_bits) == lane, held & ((1 << code_bits) - 1), 0)
        ms[me, b] = jnp.sum(found.astype(jnp.float32), axis=0, keepdims=True).astype(jnp.int32)
        return carry

    lax.fori_loop(0, tables, one_table, 0)
    ms[me, tables] = jnp.zeros((1, LANES), jnp.int32)
    ms[me, tables, :, 0:clusters] = cnt_v[...]
    onward(push, me, 2, has_low, has_high)
    onward(push, me, 1, has_low, has_high)
    live_row = ms[me, tables].astype(jnp.float32)
    cntb[...] = jnp.transpose(jnp.broadcast_to(live_row, (LANES, LANES)))[0:clusters]

    near = jnp.minimum(z, planes - 1 - z)
    long_side = jnp.where(z < planes - 1 - z, 1, -1)

    far = planes - 1 - near

    inner = near > 0
    low_side = z < planes - 1 - z

    def plane_of(k):
        at = jnp.where(inner & low_side & (k % 2 == 1), planes - k, k)
        return z + long_side * jnp.where(at <= far, at, far - at)

    def collect_of(k):
        ends = jnp.where(low_side | (k == 0) | (k == 3), k, 3 - k)
        middle = jnp.where(k == 0, 0, jnp.where(k == 1, -1, jnp.where(low_side, k - 1, 4 - k)))
        return z + long_side * jnp.where(inner, middle, ends)

    def pick_of(u, values):
        found = values[0]
        for at in range(1, len(values)):
            found = jnp.where(u == at, values[at], found)
        return found

    def chips_of(u):
        inner = near > 0
        first = pick_of(u, (1, 2, jnp.where(inner, 2, 3), 3))
        first_far = pick_of(u, (0, 0, jnp.where(inner, 1, 0), jnp.where(inner, 0, 1)))
        second = pick_of(u, (0, jnp.where(inner, 1, 0), jnp.where(inner, 0, 1), jnp.where(inner, 3, 2)))
        second_far = pick_of(u, (0, 1, 1, 1))

        def chip(k, other):
            return plane_of(k) * 2 + jnp.where(other == 1, 1 - y, y)

        return chip(first, first_far), chip(second, second_far)

    def along(k):
        return plane_of(k) * 4 + y * 2 + c

    def forward_z(k, h, act=push, wait=True):
        p = plane_of(k)
        if wait:
            arrive(along(k), h)

        @pl.when((p > z) & has_low)
        def _():
            act(along(k), h, 0, me - 4)

        @pl.when((p < z) & has_high)
        def _():
            act(along(k), h, 1, me + 4)

    def forward_y(k, h, act=push):
        act(along(k), h, 2, y_dev)

    def forward_c(k, h, act=push):
        act(along(k), h, 3, c_dev)

    def forward_plane(k, h, act=push):
        forward_y(k, h, act)
        forward_c(k, h, act)

    def relay_y(k, h):
        s = plane_of(k) * 4 + (1 - y) * 2 + c
        arrive(s, h)
        push(s, h, 3, c_dev)
        if h == 1:
            @pl.when(inner & (k == 2) & low_side)
            def _():
                push(s, h, 0, me - 4)

            @pl.when(inner & (k == 2) & jnp.logical_not(low_side))
            def _():
                push(s, h, 1, me + 4)

    def service(u, pieces):
        for h in pieces:
            @pl.when(u + 2 <= far)
            def _():
                forward_z(u + 2, h)
                forward_c(u + 2, h)

                @pl.when(inner | (u + 2 < 3) | (h != 1))
                def _():
                    forward_y(u + 2, h)

            @pl.when(u + 1 < planes)
            def _():
                relay_y(u + 1, h)

    def back_pair(g, s):
        return (
            pltpu.make_async_remote_copy(
                src_ref=sendb.at[g, pl.ds(s * short, short)],
                dst_ref=recvb.at[g, pl.ds(me * short, short)],
                send_sem=bsend.at[g], recv_sem=brecv.at[z], device_id={"owner": s},
            ),
            pltpu.make_async_remote_copy(
                src_ref=sends.at[g, s], dst_ref=recvs.at[g, me],
                send_sem=ssend.at[g], recv_sem=srecv.at[z], device_id={"owner": s},
            ),
        )

    def back_arrive(p, first, owners):
        for ref, sem, each in ((recvb, brecv, short), (recvs, srecv, 1)):
            cut = pl.ds(first * each, owners * each)
            pltpu.make_async_remote_copy(
                src_ref=ref.at[:, cut], dst_ref=ref.at[:, cut],
                send_sem=bsend.at[0], recv_sem=sem.at[p], device_id={"owner": c_dev},
            ).wait_recv()

    def compute(k):
        chips = chips_of(k)
        codes = jnp.concatenate(
            [join(ms[2 * chip, me // 2], ms[2 * chip + 1, me // 2]) for chip in chips], axis=1
        )
        cluster = codes >> q_bits
        block_of = lax.broadcasted_iota(jnp.int32, (1, wide), 1) // cap
        source = (codes & (per_device - 1)) + block_of * per_device
        pick = jnp.where(
            lax.broadcasted_iota(jnp.int32, (rows, wide), 0) == source, 1.0, 0.0
        ).astype(jnp.bfloat16)
        block = jnp.concatenate(
            [qs[pl.ds(2 * chip, 2)].reshape(2 * per_device, width) for chip in chips], axis=0
        )
        rows_v[...] = lax.dot_general(
            block, pick, (((0,), (0,)), ((), ())), preferred_element_type=jnp.float32
        ).astype(jnp.bfloat16)
        count_of = jnp.concatenate([cntb[...], cntb[...]], axis=1)

        def one_half(g, carry):
            @pl.when(k == 0)
            def _():
                pltpu.make_async_copy(pass_v.at[g], pass_v.at[g], pass_sem.at[g]).wait()

            direct = lax.dot_general(
                pass_v[g], rows_v[...], (((1,), (0,)), ((), ())), preferred_element_type=jnp.float32
            )
            total = direct[:half]
            for u in range(1, clusters):
                total = jnp.where(
                    jnp.broadcast_to(cluster, (half, wide)) == u, direct[u * half : (u + 1) * half], total
                )
            acc[...] = total
            mine = lax.broadcasted_iota(jnp.int32, (clusters, wide), 0) == cluster
            term = jnp.sum(jnp.where(mine, direct[clusters * half :], 0.0), axis=0, keepdims=True)
            live = jnp.sum(jnp.where(mine, count_of, 0.0), axis=0, keepdims=True).astype(jnp.int32)
            place = lax.broadcasted_iota(jnp.int32, (half, wide), 0) + g * half
            value = jnp.where(place < live, acc[...] + term, 0.0)
            top = jnp.maximum(jnp.max(jnp.abs(value), axis=0, keepdims=True), 1e-30)
            coded = jnp.round(value * (TOP / top)).astype(jnp.int32)
            unit = top * (1.0 / TOP)
            for b, chip in enumerate(chips):
                part = coded[:, b * LANES : (b + 1) * LANES]
                packed = (pltpu.roll(part, LANES - short, 1) << 16) | (part & 0xFFFF)
                turned = jnp.transpose(packed)
                lane_unit = jnp.broadcast_to(unit[:, b * LANES : (b + 1) * LANES], (8, LANES))
                other = pltpu.roll(lane_unit, cap, 1)
                for i in range(2):
                    sendb[g, pl.ds((2 * chip + i) * short, short)] = turned[i * cap : i * cap + short]
                    sends[g, 2 * chip + i] = jnp.where((lane_row < cap) == (i == 0), lane_unit, other)[0:1]
            for i in range(4):
                s = 2 * chips[i // 2] + i % 2

                @pl.when(s == me)
                def _():
                    recvb[g, pl.ds(me * short, short)] = sendb[g, pl.ds(me * short, short)]
                    recvs[g, me] = sends[g, me]

                @pl.when(s != me)
                def _():
                    for copy in back_pair(g, s):
                        copy.start()

            @pl.when((g == 0) == ((k != 2) | (near > 0)))
            def _():
                service(k, (0, 2, 1))

            return carry

        lax.fori_loop(0, 2, one_half, 0)

    lead_k = jnp.where(inner & low_side, planes - 1, 1)
    for h in (0, 2, 1):
        forward_z(lead_k, h)
        forward_plane(lead_k, h)

        @pl.when(inner)
        def _():
            forward_z(planes - lead_k, h)
            forward_plane(planes - lead_k, h)

        relay_y(0, h)

    count_copy = pltpu.make_async_copy(ms.at[:, tables], cnt_s, load_sem.at[0])

    def step(k, carry):
        for chip in chips_of(k):
            for h in range(3):
                arrive(2 * chip + (1 - c), h)

        @pl.when(k == planes - 1)
        def _():
            count_copy.start()

        compute(k)
        return carry

    lax.fori_loop(0, planes, step, 0)

    count_copy.wait()

    def one_owner(o, seen):
        for l in range(clusters):
            seen = jnp.where(probe_v[...] == o * clusters + l, cnt_s[o, 0, l], seen)
        return seen

    seen = lax.fori_loop(0, n, one_owner, jnp.zeros((probe_count, per_device), jnp.int32))
    vis_ref[...] = jnp.sum(seen.astype(jnp.float32), axis=0, keepdims=True).astype(jnp.int32)

    def collect(k, carry):
        p = collect_of(k)
        base = p * 4
        @pl.when(p == z)
        def _():
            back_arrive(p, base, 3)

        @pl.when(p != z)
        def _():
            back_arrive(p, base, 4)

        quarter = lax.broadcasted_iota(jnp.int32, (8, LANES), 1) // short
        columns = []
        for g in range(2):
            straight = [jnp.broadcast_to(recvs[g, base + i], (8, LANES)) for i in range(4)]
            shifted = [pltpu.roll(row, short, 1) for row in straight]
            held = recvb[g, pl.ds(base * short, LANES)]
            halves = []
            for high in range(2):
                unit = jnp.zeros((8, LANES), jnp.float32)
                for i in range(4):
                    unit = jnp.where(quarter == i, straight[i] if i % 2 == high else shifted[i], unit)
                units = jnp.transpose(jnp.broadcast_to(unit[0:1], (LANES, LANES)))
                number = held >> 16 if high else (held << 16) >> 16
                halves.append(number.astype(jnp.float32) * units)
            columns.append(jnp.concatenate(halves, axis=0))
        value = jnp.concatenate(columns, axis=1)
        upper_part = value.astype(jnp.bfloat16)
        lower_part = (value - upper_part.astype(jnp.float32)).astype(jnp.bfloat16)
        at = slots[...] >> code_bits
        lane = lax.broadcasted_iota(jnp.int32, (pairs, LANES), 1)
        lane = (lane // short + base) * cap + lane % short
        chosen = jnp.concatenate(
            [jnp.where(at == lane + b * short, 1.0, 0.0).astype(jnp.bfloat16) for b in range(2)], axis=1
        )
        part = jnp.dot(chosen, upper_part, preferred_element_type=jnp.float32) + jnp.dot(
            chosen, lower_part, preferred_element_type=jnp.float32
        )

        @pl.when(k == 0)
        def _():
            out_ref[...] = part

        @pl.when(k > 0)
        def _():
            out_ref[...] += part

        return carry

    lax.fori_loop(0, planes, collect, 0)

    @pl.when(inner)
    def _():
        drain(0, planes + 1, 2 * planes + 3)
        drain(1, planes, 2 * planes)

    @pl.when(jnp.logical_not(inner))
    def _():
        drain(0, 1, 2)
        drain(1, planes, 2 * planes - 1)

    drain(2, 2 * planes, 4 * planes)
    for g in range(2):
        for ref, sem, each in ((sendb, bsend, short), (sends, ssend, 1)):
            cut = ref.at[g, pl.ds(0, (n - 1) * each)]
            pltpu.make_async_remote_copy(
                src_ref=cut, dst_ref=cut, send_sem=sem.at[g], recv_sem=brecv.at[0],
                device_id={"owner": c_dev},
            ).wait_send()


def deliver(scores_ref, visits_ref, scores_out, visits_out, sem):
    copies = (
        pltpu.make_async_copy(scores_ref, scores_out, sem.at[0]),
        pltpu.make_async_copy(visits_ref, visits_out, sem.at[1]),
    )
    for copy in copies:
        copy.start()
    for copy in copies:
        copy.wait()


def fused_body(queries, probes, passages, centroids, counts):
    n = lax.axis_size("owner")
    per_device, probe_count = probes.shape
    clusters, span, width = passages.shape
    cap = 2 * per_device * probe_count // n
    pairs = per_device * probe_count
    tables = n * cap // LANES
    wide = 4 * cap
    vmem = pl.BlockSpec(memory_space=pltpu.VMEM)
    hbm = pl.BlockSpec(memory_space=pltpu.HBM)
    dma = pltpu.SemaphoreType.DMA
    scores, visits = pl.pallas_call(
        lambda *refs: owner_kernel(n, *refs),
        out_shape=(
            jax.ShapeDtypeStruct((pairs, span), jnp.float32),
            jax.ShapeDtypeStruct((1, per_device), jnp.int32),
        ),
        in_specs=[hbm] * 5,
        out_specs=(vmem, vmem),
        scratch_shapes=[
            pltpu.VMEM((2, clusters * span // 2 + clusters, width), jnp.bfloat16),
            pltpu.VMEM((n, per_device, width), jnp.bfloat16),
            pltpu.VMEM((1, clusters), jnp.int32),
            pltpu.VMEM((probe_count, per_device), jnp.int32),
            pltpu.VMEM((n, tables + 1, 1, LANES), jnp.int32),
            pltpu.VMEM((pairs, LANES), jnp.int32),
            pltpu.VMEM((width, wide), jnp.bfloat16),
            pltpu.VMEM((span // 2, wide), jnp.float32),
            pltpu.VMEM((clusters, LANES), jnp.float32),
            pltpu.VMEM((2, n * cap // 2, LANES), jnp.int32),
            pltpu.VMEM((2, n, 1, LANES), jnp.float32),
            pltpu.VMEM((2, n * cap // 2, LANES), jnp.int32),
            pltpu.VMEM((2, n, 1, LANES), jnp.float32),
            pltpu.SMEM((n, 1, LANES), jnp.int32),
            dma((2,)),
            dma((3,)),
            dma((3,)),
            dma((3,)),
            dma((n, 2)),
            dma((n,)),
            dma((2,)),
            dma((2,)),
            dma((n // 4,)),
            dma((n // 4,)),
        ],
        compiler_params=pltpu.CompilerParams(
            collective_id=0, has_side_effects=True, vmem_limit_bytes=48 * 2**20
        ),
    )(*[pltpu.with_memory_space_constraint(v, pltpu.HBM) for v in (queries, probes.T, passages, centroids, counts.reshape(1, clusters))])
    scores, visits = pl.pallas_call(
        deliver,
        out_shape=(
            jax.ShapeDtypeStruct((pairs, span), jnp.float32),
            jax.ShapeDtypeStruct((1, per_device), jnp.int32),
        ),
        in_specs=[vmem] * 2,
        out_specs=(pl.BlockSpec(memory_space=pl.ANY), pl.BlockSpec(memory_space=pl.ANY)),
        scratch_shapes=[dma((2,))],
        compiler_params=pltpu.CompilerParams(vmem_limit_bytes=2**20),
    )(*[pltpu.with_memory_space_constraint(v, pltpu.VMEM) for v in (scores, visits)])
    return scores.reshape(per_device, probe_count, span), visits.reshape(per_device)


def power_of_two(value):
    return value > 0 and value & (value - 1) == 0


def body(queries, probes, passages, centroids, counts):
    n = lax.axis_size("owner")
    per_device, probe_count = probes.shape
    clusters, span, width = passages.shape
    cap = 2 * per_device * probe_count // n
    held = 2 * width * (clusters * span + n * per_device)
    fits = (
        n == 16 and clusters % 16 == 0 and 2 * cap == LANES and n * probe_count == LANES and span == 2 * LANES
        and power_of_two(clusters) and power_of_two(per_device) and power_of_two(probe_count)
        and clusters <= LANES and per_device == cap
        and clusters * per_device * n * cap < 2**23 and width % LANES == 0 and held < 32 * 2**20
    )
    chosen = fused_body if fits else routed_body
    return chosen(queries, probes, passages, centroids, counts)


def solution(mesh):
    in_specs = (
        P(("groups", "owner"), None),
        P(("groups", "owner"), None),
        P("owner", None, None),
        P("owner", None),
        P("owner"),
    )
    out_specs = (P(("groups", "owner"), None, None), P(("groups", "owner")))
    return jax.shard_map(body, mesh=mesh, in_specs=in_specs, out_specs=out_specs, check_vma=False)
```

```python
import jax
import jax.numpy as jnp
from jax import lax
from jax.experimental import pallas as pl
from jax.experimental.pallas import tpu as pltpu
from jax.sharding import PartitionSpec as P


def routed_body(queries, probes, passages, centroids, counts):
    owner_count = lax.axis_size("owner")
    per_device, probe_count = probes.shape
    local_count, block_span, feature_width = passages.shape
    capacity = 2 * per_device * probe_count // owner_count
    pair_count = per_device * probe_count
    passage_blocks = jnp.transpose(passages, (0, 2, 1))
    flat_probes = probes.reshape(-1)
    target_owner = flat_probes // local_count
    target_local = flat_probes % local_count
    owner_hits = (
        target_owner[:, None] == jnp.arange(owner_count, dtype=jnp.int32)[None, :]
    ).astype(jnp.int32)
    slot_rank = jnp.sum((jnp.cumsum(owner_hits, axis=0) - owner_hits) * owner_hits, axis=1)
    slot_index = target_owner * capacity + slot_rank
    pair_ids = jnp.arange(pair_count, dtype=jnp.int32)
    slot_match = slot_index[None, :] == jnp.arange(owner_count * capacity, dtype=jnp.int32)[:, None]
    slot_filled = jnp.any(slot_match, axis=1)
    source_pair = jnp.sum(jnp.where(slot_match, pair_ids[None, :], 0), axis=1)
    send_rows = jnp.where(
        slot_filled[:, None], queries[source_pair // probe_count], jnp.zeros((), jnp.bfloat16)
    )
    send_ids = jnp.where(slot_filled, target_local[source_pair], -1)
    query_rows = lax.all_to_all(
        send_rows.reshape(owner_count, capacity, feature_width),
        "owner",
        split_axis=0,
        concat_axis=0,
        tiled=True,
    )
    cluster_ids = lax.all_to_all(
        send_ids.reshape(owner_count, capacity), "owner", split_axis=0, concat_axis=0, tiled=True
    )
    source_count, slot_count = cluster_ids.shape
    row_total = source_count * slot_count
    flat_rows = query_rows.reshape(row_total, feature_width)
    flat_ids = cluster_ids.reshape(-1)
    group_ids = jnp.where(flat_ids < 0, 0, flat_ids).astype(jnp.int32)
    cluster_pick = flat_ids[:, None] == jnp.arange(local_count, dtype=jnp.int32)[None, :]
    live_sizes = jnp.sum(jnp.where(cluster_pick, counts[None, :], 0), axis=1)
    group_pick = group_ids[:, None] == jnp.arange(local_count, dtype=jnp.int32)[None, :]
    group_sizes = jnp.sum(group_pick.astype(jnp.int32), axis=0)
    order = jnp.argsort(group_ids, stable=True)
    undo_order = jnp.argsort(order, stable=True)
    sorted_rows = flat_rows[order]
    sorted_scores = lax.ragged_dot(
        sorted_rows, passage_blocks, group_sizes, preferred_element_type=jnp.float32
    )
    own_scores = sorted_scores[undo_order]
    centre_term = jnp.einsum(
        "rd,rd->r", flat_rows, centroids[group_ids], preferred_element_type=jnp.float32
    )
    live_mask = jnp.arange(block_span, dtype=jnp.int32)[None, :] < live_sizes[:, None]
    masked_scores = jnp.where(live_mask, own_scores + centre_term[:, None], 0.0)
    back_scores = lax.all_to_all(
        masked_scores.reshape(source_count, slot_count, block_span),
        "owner",
        split_axis=0,
        concat_axis=0,
        tiled=True,
    )
    back_sizes = lax.all_to_all(
        live_sizes.astype(jnp.float32).reshape(source_count, slot_count),
        "owner",
        split_axis=0,
        concat_axis=0,
        tiled=True,
    )
    flat_scores = back_scores.reshape(owner_count * capacity, block_span)
    scores = flat_scores[slot_index].reshape(per_device, probe_count, block_span)
    pair_sizes = back_sizes.reshape(-1)[slot_index].reshape(per_device, probe_count)
    visits = jnp.sum(pair_sizes, axis=1).astype(jnp.int32)
    return (scores, visits)


LANES = 128
TOP = 32767.0


def owner_kernel(
    n, q_hbm, probe_hbm, pass_hbm, cent_hbm, cnt_hbm,
    out_ref, vis_ref,
    pass_v, qs, cnt_v, probe_v, ms, slots, rows_v, acc, cntb, sendb, sends, recvb, recvs, cnt_s,
    pass_sem, load_sem, qsend, msend, qrecv, mrecv, bsend, ssend, brecv, srecv,
):
    clusters, width = cent_hbm.shape
    span = pass_hbm.shape[1]
    probe_count, per_device = probe_v.shape
    pairs = probe_count * per_device
    planes = n // 4
    rows = 4 * per_device
    tables = ms.shape[1] - 1
    cap = LANES // 2
    wide = 4 * cap
    half = span // 2
    short = cap // 2
    piece = per_device // 2
    code_bits = (clusters * per_device).bit_length() - 1
    q_bits = per_device.bit_length() - 1
    cl_bits = clusters.bit_length() - 1
    me = lax.axis_index("owner")
    z = me // 4
    y = (me // 2) % 2
    c = me % 2
    y_dev = z * 4 + (1 - y) * 2 + c
    c_dev = z * 4 + y * 2 + (1 - c)
    has_low = z > 0
    has_high = z < planes - 1

    loads = [
        pltpu.make_async_copy(q_hbm, qs.at[me], load_sem.at[0]),
        pltpu.make_async_copy(probe_hbm, probe_v, load_sem.at[1]),
        pltpu.make_async_copy(cnt_hbm, cnt_v, load_sem.at[2]),
    ]
    for copy in loads:
        copy.start()

    barrier = pltpu.get_barrier_semaphore()

    def greet(dev):
        pl.semaphore_signal(barrier, inc=1, device_id={"owner": dev})

    greet(y_dev)
    greet(c_dev)

    @pl.when(has_low)
    def _():
        greet(me - 4)

    @pl.when(has_high)
    def _():
        greet(me + 4)

    def passage_copies(g):
        return [
            pltpu.make_async_copy(
                pass_hbm.at[k, pl.ds(g * half, half)], pass_v.at[g, pl.ds(k * half, half)], pass_sem.at[g]
            )
            for k in range(clusters)
        ] + [
            pltpu.make_async_copy(cent_hbm, pass_v.at[g, pl.ds(clusters * half, clusters)], pass_sem.at[g])
        ]

    for g in range(2):
        for copy in passage_copies(g):
            copy.start()

    loads[0].wait()
    pl.semaphore_wait(barrier, 2 + jnp.where(has_low, 1, 0) + jnp.where(has_high, 1, 0))

    def chunk(s, h, target, dev):
        if h == 2:
            return pltpu.make_async_remote_copy(
                src_ref=ms.at[s], dst_ref=ms.at[s],
                send_sem=msend.at[max(target - 1, 0)], recv_sem=mrecv.at[s], device_id={"owner": dev},
            )
        cut = pl.ds(h * piece, piece)
        return pltpu.make_async_remote_copy(
            src_ref=qs.at[s, cut], dst_ref=qs.at[s, cut],
            send_sem=qsend.at[max(target - 1, 0)], recv_sem=qrecv.at[n + s // 2 if target == 3 else s // 2 * 2 + h], device_id={"owner": dev},
        )

    def push(s, h, target, dev):
        chunk(s, h, target, dev).start()

    def drain(way, blocks, halves):
        for cut, sem in (
            (pass_v.at[0, pl.ds(0, halves * piece)], qsend),
            (ms.at[pl.ds(0, blocks)], msend),
        ):
            pltpu.make_async_remote_copy(
                src_ref=cut, dst_ref=cut, send_sem=sem.at[way], recv_sem=mrecv.at[0],
                device_id={"owner": c_dev},
            ).wait_send()

    def arrive(s, h):
        chunk(s, h, 0, c_dev).wait_recv()

    def onward(act, s, h, low, high):
        @pl.when(low)
        def _():
            act(s, h, 0, me - 4)

        @pl.when(high)
        def _():
            act(s, h, 1, me + 4)

        act(s, h, 2, y_dev)
        act(s, h, 3, c_dev)

    onward(push, me, 0, has_low, has_high)

    for copy in loads[1:]:
        copy.wait()

    def lower(row):
        return jnp.where(c == 1, pltpu.roll(row, cap, 1), row)

    def upper(row):
        return jnp.where(c == 1, row, pltpu.roll(row, cap, 1))

    lane_row = lax.broadcasted_iota(jnp.int32, (8, LANES), 1)

    def join(first, second):
        first = jnp.broadcast_to(first, (8, LANES))
        second = jnp.broadcast_to(second, (8, LANES))
        return jnp.where(lane_row < cap, lower(first), upper(second))[0:1]

    probes = probe_v[...]
    target = probes >> cl_bits
    local = probes & (clusters - 1)
    hits = jnp.concatenate(
        [jnp.where(target == o, 1.0, 0.0).astype(jnp.float32) for o in range(n)], axis=0
    ).astype(jnp.bfloat16)
    big = n * probe_count
    r_iota = lax.broadcasted_iota(jnp.int32, (big, big), 0)
    c_iota = lax.broadcasted_iota(jnp.int32, (big, big), 1)
    p_bits = probe_count.bit_length() - 1
    earlier = jnp.where(
        ((r_iota >> p_bits) == (c_iota >> p_bits)) & (c_iota < r_iota), 1.0, 0.0
    ).astype(jnp.bfloat16)
    before = jnp.where(
        lax.broadcasted_iota(jnp.int32, (per_device, per_device), 0)
        < lax.broadcasted_iota(jnp.int32, (per_device, per_device), 1), 1.0, 0.0,
    ).astype(jnp.bfloat16)
    lead = jnp.dot(earlier, hits, preferred_element_type=jnp.float32).astype(jnp.bfloat16)
    ranks = jnp.dot(hits, before, preferred_element_type=jnp.float32) + jnp.dot(
        lead, jnp.ones((per_device, per_device), jnp.bfloat16), preferred_element_type=jnp.float32
    )
    rank = jnp.zeros((probe_count, per_device), jnp.float32)
    for o in range(n):
        rank = jnp.where(target == o, ranks[o * probe_count : (o + 1) * probe_count], rank)
    slot = target * cap + rank.astype(jnp.int32)
    code = local * per_device + lax.broadcasted_iota(jnp.int32, (probe_count, per_device), 1)
    word = (slot << code_bits) | code
    for q in range(per_device):
        slots[q * probe_count : (q + 1) * probe_count, :] = jnp.broadcast_to(
            word[:, q : q + 1], (probe_count, LANES)
        )

    def one_table(b, carry):
        lane = lax.broadcasted_iota(jnp.int32, (pairs, LANES), 1) + b * LANES
        held = slots[...]
        found = jnp.where((held >> code_bits) == lane, held & ((1 << code_bits) - 1), 0)
        ms[me, b] = jnp.sum(found.astype(jnp.float32), axis=0, keepdims=True).astype(jnp.int32)
        return carry

    lax.fori_loop(0, tables, one_table, 0)
    ms[me, tables] = jnp.zeros((1, LANES), jnp.int32)
    ms[me, tables, :, 0:clusters] = cnt_v[...]
    onward(push, me, 2, has_low, has_high)
    onward(push, me, 1, has_low, has_high)
    live_row = ms[me, tables].astype(jnp.float32)
    cntb[...] = jnp.transpose(jnp.broadcast_to(live_row, (LANES, LANES)))[0:clusters]

    near = jnp.minimum(z, planes - 1 - z)
    long_side = jnp.where(z < planes - 1 - z, 1, -1)

    far = planes - 1 - near

    inner = near > 0
    low_side = z < planes - 1 - z

    def plane_of(k):
        at = jnp.where(inner & low_side & (k % 2 == 1), planes - k, k)
        return z + long_side * jnp.where(at <= far, at, far - at)

    def collect_of(k):
        ends = jnp.where(low_side | (k == 0) | (k == 3), k, 3 - k)
        middle = jnp.where(k == 0, 0, jnp.where(k == 1, -1, jnp.where(low_side, k - 1, 4 - k)))
        return z + long_side * jnp.where(inner, middle, ends)

    def pick_of(u, values):
        found = values[0]
        for at in range(1, len(values)):
            found = jnp.where(u == at, values[at], found)
        return found

    def chips_of(u):
        inner = near > 0
        first = pick_of(u, (1, 2, jnp.where(inner, 2, 3), 3))
        first_far = pick_of(u, (0, 0, jnp.where(inner, 1, 0), jnp.where(inner, 0, 1)))
        second = pick_of(u, (0, jnp.where(inner, 1, 0), jnp.where(inner, 0, 1), jnp.where(inner, 3, 2)))
        second_far = pick_of(u, (0, 1, 1, 1))

        def chip(k, other):
            return plane_of(k) * 2 + jnp.where(other == 1, 1 - y, y)

        return chip(first, first_far), chip(second, second_far)

    def along(k):
        return plane_of(k) * 4 + y * 2 + c

    def forward_z(k, h, act=push, wait=True):
        p = plane_of(k)
        if wait:
            arrive(along(k), h)

        @pl.when((p > z) & has_low)
        def _():
            act(along(k), h, 0, me - 4)

        @pl.when((p < z) & has_high)
        def _():
            act(along(k), h, 1, me + 4)

    def forward_y(k, h, act=push):
        act(along(k), h, 2, y_dev)

    def forward_c(k, h, act=push):
        act(along(k), h, 3, c_dev)

    def forward_plane(k, h, act=push):
        forward_y(k, h, act)
        forward_c(k, h, act)

    def relay_y(k, h):
        s = plane_of(k) * 4 + (1 - y) * 2 + c
        arrive(s, h)
        push(s, h, 3, c_dev)
        if h == 1:
            @pl.when(inner & (k == 2) & low_side)
            def _():
                push(s, h, 0, me - 4)

            @pl.when(inner & (k == 2) & jnp.logical_not(low_side))
            def _():
                push(s, h, 1, me + 4)

    def service(u, pieces):
        for h in pieces:
            @pl.when(u + 2 <= far)
            def _():
                forward_z(u + 2, h)
                forward_c(u + 2, h)

                @pl.when(inner | (u + 2 < 3) | (h != 1))
                def _():
                    forward_y(u + 2, h)

            @pl.when(u + 1 < planes)
            def _():
                relay_y(u + 1, h)

    def back_pair(g, s):
        return (
            pltpu.make_async_remote_copy(
                src_ref=sendb.at[g, pl.ds(s * short, short)],
                dst_ref=recvb.at[g, pl.ds(me * short, short)],
                send_sem=bsend.at[g], recv_sem=brecv.at[z], device_id={"owner": s},
            ),
            pltpu.make_async_remote_copy(
                src_ref=sends.at[g, s], dst_ref=recvs.at[g, me],
                send_sem=ssend.at[g], recv_sem=srecv.at[z], device_id={"owner": s},
            ),
        )

    def back_arrive(p, first, owners):
        for ref, sem, each in ((recvb, brecv, short), (recvs, srecv, 1)):
            cut = pl.ds(first * each, owners * each)
            pltpu.make_async_remote_copy(
                src_ref=ref.at[:, cut], dst_ref=ref.at[:, cut],
                send_sem=bsend.at[0], recv_sem=sem.at[p], device_id={"owner": c_dev},
            ).wait_recv()

    def compute(k):
        chips = chips_of(k)
        codes = jnp.concatenate(
            [join(ms[2 * chip, me // 2], ms[2 * chip + 1, me // 2]) for chip in chips], axis=1
        )
        cluster = codes >> q_bits
        block_of = lax.broadcasted_iota(jnp.int32, (1, wide), 1) // cap
        source = (codes & (per_device - 1)) + block_of * per_device
        pick = jnp.where(
            lax.broadcasted_iota(jnp.int32, (rows, wide), 0) == source, 1.0, 0.0
        ).astype(jnp.bfloat16)
        block = jnp.concatenate(
            [qs[pl.ds(2 * chip, 2)].reshape(2 * per_device, width) for chip in chips], axis=0
        )
        rows_v[...] = lax.dot_general(
            block, pick, (((0,), (0,)), ((), ())), preferred_element_type=jnp.float32
        ).astype(jnp.bfloat16)
        count_of = jnp.concatenate([cntb[...], cntb[...]], axis=1)

        def one_half(g, carry):
            @pl.when(k == 0)
            def _():
                pltpu.make_async_copy(pass_v.at[g], pass_v.at[g], pass_sem.at[g]).wait()

            direct = lax.dot_general(
                pass_v[g], rows_v[...], (((1,), (0,)), ((), ())), preferred_element_type=jnp.float32
            )
            total = direct[:half]
            for u in range(1, clusters):
                total = jnp.where(
                    jnp.broadcast_to(cluster, (half, wide)) == u, direct[u * half : (u + 1) * half], total
                )
            acc[...] = total
            mine = lax.broadcasted_iota(jnp.int32, (clusters, wide), 0) == cluster
            term = jnp.sum(jnp.where(mine, direct[clusters * half :], 0.0), axis=0, keepdims=True)
            live = jnp.sum(jnp.where(mine, count_of, 0.0), axis=0, keepdims=True).astype(jnp.int32)
            place = lax.broadcasted_iota(jnp.int32, (half, wide), 0) + g * half
            value = jnp.where(place < live, acc[...] + term, 0.0)
            top = jnp.maximum(jnp.max(jnp.abs(value), axis=0, keepdims=True), 1e-30)
            coded = jnp.round(value * (TOP / top)).astype(jnp.int32)
            unit = top * (1.0 / TOP)
            for b, chip in enumerate(chips):
                part = coded[:, b * LANES : (b + 1) * LANES]
                packed = (pltpu.roll(part, LANES - short, 1) << 16) | (part & 0xFFFF)
                turned = jnp.transpose(packed)
                lane_unit = jnp.broadcast_to(unit[:, b * LANES : (b + 1) * LANES], (8, LANES))
                other = pltpu.roll(lane_unit, cap, 1)
                for i in range(2):
                    sendb[g, pl.ds((2 * chip + i) * short, short)] = turned[i * cap : i * cap + short]
                    sends[g, 2 * chip + i] = jnp.where((lane_row < cap) == (i == 0), lane_unit, other)[0:1]
            for i in range(4):
                s = 2 * chips[i // 2] + i % 2

                @pl.when(s == me)
                def _():
                    recvb[g, pl.ds(me * short, short)] = sendb[g, pl.ds(me * short, short)]
                    recvs[g, me] = sends[g, me]

                @pl.when(s != me)
                def _():
                    for copy in back_pair(g, s):
                        copy.start()

            @pl.when((g == 0) == ((k != 2) | (near > 0)))
            def _():
                service(k, (0, 2, 1))

            return carry

        lax.fori_loop(0, 2, one_half, 0)

    lead_k = jnp.where(inner & low_side, planes - 1, 1)
    for h in (0, 2, 1):
        forward_z(lead_k, h)
        forward_plane(lead_k, h)

        @pl.when(inner)
        def _():
            forward_z(planes - lead_k, h)
            forward_plane(planes - lead_k, h)

        relay_y(0, h)

    count_copy = pltpu.make_async_copy(ms.at[:, tables], cnt_s, load_sem.at[0])

    def step(k, carry):
        for chip in chips_of(k):
            s = 2 * chip + (1 - c)
            pltpu.make_async_remote_copy(
                src_ref=qs.at[s], dst_ref=qs.at[s], send_sem=qsend.at[2],
                recv_sem=qrecv.at[n + s // 2], device_id={"owner": c_dev},
            ).wait_recv()
            arrive(s, 2)

        @pl.when(k == planes - 1)
        def _():
            count_copy.start()

        compute(k)
        return carry

    lax.fori_loop(0, planes, step, 0)

    count_copy.wait()

    def one_owner(o, seen):
        for l in range(clusters):
            seen = jnp.where(probe_v[...] == o * clusters + l, cnt_s[o, 0, l], seen)
        return seen

    seen = lax.fori_loop(0, n, one_owner, jnp.zeros((probe_count, per_device), jnp.int32))
    vis_ref[...] = jnp.sum(seen.astype(jnp.float32), axis=0, keepdims=True).astype(jnp.int32)

    def collect(k, carry):
        p = collect_of(k)
        base = p * 4
        @pl.when(p == z)
        def _():
            back_arrive(p, base, 3)

        @pl.when(p != z)
        def _():
            back_arrive(p, base, 4)

        quarter = lax.broadcasted_iota(jnp.int32, (8, LANES), 1) // short
        columns = []
        for g in range(2):
            straight = [jnp.broadcast_to(recvs[g, base + i], (8, LANES)) for i in range(4)]
            shifted = [pltpu.roll(row, short, 1) for row in straight]
            held = recvb[g, pl.ds(base * short, LANES)]
            halves = []
            for high in range(2):
                unit = jnp.zeros((8, LANES), jnp.float32)
                for i in range(4):
                    unit = jnp.where(quarter == i, straight[i] if i % 2 == high else shifted[i], unit)
                units = jnp.transpose(jnp.broadcast_to(unit[0:1], (LANES, LANES)))
                number = held >> 16 if high else (held << 16) >> 16
                halves.append(number.astype(jnp.float32) * units)
            columns.append(jnp.concatenate(halves, axis=0))
        value = jnp.concatenate(columns, axis=1)
        upper_part = value.astype(jnp.bfloat16)
        lower_part = (value - upper_part.astype(jnp.float32)).astype(jnp.bfloat16)
        at = slots[...] >> code_bits
        lane = lax.broadcasted_iota(jnp.int32, (pairs, LANES), 1)
        lane = (lane // short + base) * cap + lane % short
        chosen = jnp.concatenate(
            [jnp.where(at == lane + b * short, 1.0, 0.0).astype(jnp.bfloat16) for b in range(2)], axis=1
        )
        part = jnp.dot(chosen, upper_part, preferred_element_type=jnp.float32) + jnp.dot(
            chosen, lower_part, preferred_element_type=jnp.float32
        )

        @pl.when(k == 0)
        def _():
            out_ref[...] = part

        @pl.when(k > 0)
        def _():
            out_ref[...] += part

        return carry

    lax.fori_loop(0, planes, collect, 0)

    @pl.when(inner)
    def _():
        drain(0, planes + 1, 2 * planes + 3)
        drain(1, planes, 2 * planes)

    @pl.when(jnp.logical_not(inner))
    def _():
        drain(0, 1, 2)
        drain(1, planes, 2 * planes - 1)

    drain(2, 2 * planes, 4 * planes)
    for g in range(2):
        for ref, sem, each in ((sendb, bsend, short), (sends, ssend, 1)):
            cut = ref.at[g, pl.ds(0, (n - 1) * each)]
            pltpu.make_async_remote_copy(
                src_ref=cut, dst_ref=cut, send_sem=sem.at[g], recv_sem=brecv.at[0],
                device_id={"owner": c_dev},
            ).wait_send()


def deliver(scores_ref, visits_ref, scores_out, visits_out, sem):
    copies = (
        pltpu.make_async_copy(scores_ref, scores_out, sem.at[0]),
        pltpu.make_async_copy(visits_ref, visits_out, sem.at[1]),
    )
    for copy in copies:
        copy.start()
    for copy in copies:
        copy.wait()


def fused_body(queries, probes, passages, centroids, counts):
    n = lax.axis_size("owner")
    per_device, probe_count = probes.shape
    clusters, span, width = passages.shape
    cap = 2 * per_device * probe_count // n
    pairs = per_device * probe_count
    tables = n * cap // LANES
    wide = 4 * cap
    vmem = pl.BlockSpec(memory_space=pltpu.VMEM)
    hbm = pl.BlockSpec(memory_space=pltpu.HBM)
    dma = pltpu.SemaphoreType.DMA
    scores, visits = pl.pallas_call(
        lambda *refs: owner_kernel(n, *refs),
        out_shape=(
            jax.ShapeDtypeStruct((pairs, span), jnp.float32),
            jax.ShapeDtypeStruct((1, per_device), jnp.int32),
        ),
        in_specs=[hbm] * 5,
        out_specs=(vmem, vmem),
        scratch_shapes=[
            pltpu.VMEM((2, clusters * span // 2 + clusters, width), jnp.bfloat16),
            pltpu.VMEM((n, per_device, width), jnp.bfloat16),
            pltpu.VMEM((1, clusters), jnp.int32),
            pltpu.VMEM((probe_count, per_device), jnp.int32),
            pltpu.VMEM((n, tables + 1, 1, LANES), jnp.int32),
            pltpu.VMEM((pairs, LANES), jnp.int32),
            pltpu.VMEM((width, wide), jnp.bfloat16),
            pltpu.VMEM((span // 2, wide), jnp.float32),
            pltpu.VMEM((clusters, LANES), jnp.float32),
            pltpu.VMEM((2, n * cap // 2, LANES), jnp.int32),
            pltpu.VMEM((2, n, 1, LANES), jnp.float32),
            pltpu.VMEM((2, n * cap // 2, LANES), jnp.int32),
            pltpu.VMEM((2, n, 1, LANES), jnp.float32),
            pltpu.SMEM((n, 1, LANES), jnp.int32),
            dma((2,)),
            dma((3,)),
            dma((3,)),
            dma((3,)),
            dma((n + n // 2,)),
            dma((n,)),
            dma((2,)),
            dma((2,)),
            dma((n // 4,)),
            dma((n // 4,)),
        ],
        compiler_params=pltpu.CompilerParams(
            collective_id=0, has_side_effects=True, vmem_limit_bytes=48 * 2**20
        ),
    )(*[pltpu.with_memory_space_constraint(v, pltpu.HBM) for v in (queries, probes.T, passages, centroids, counts.reshape(1, clusters))])
    scores, visits = pl.pallas_call(
        deliver,
        out_shape=(
            jax.ShapeDtypeStruct((pairs, span), jnp.float32),
            jax.ShapeDtypeStruct((1, per_device), jnp.int32),
        ),
        in_specs=[vmem] * 2,
        out_specs=(pl.BlockSpec(memory_space=pl.ANY), pl.BlockSpec(memory_space=pl.ANY)),
        scratch_shapes=[dma((2,))],
        compiler_params=pltpu.CompilerParams(vmem_limit_bytes=2**20),
    )(*[pltpu.with_memory_space_constraint(v, pltpu.VMEM) for v in (scores, visits)])
    return scores.reshape(per_device, probe_count, span), visits.reshape(per_device)


def power_of_two(value):
    return value > 0 and value & (value - 1) == 0


def body(queries, probes, passages, centroids, counts):
    n = lax.axis_size("owner")
    per_device, probe_count = probes.shape
    clusters, span, width = passages.shape
    cap = 2 * per_device * probe_count // n
    held = 2 * width * (clusters * span + n * per_device)
    fits = (
        n == 16 and clusters % 16 == 0 and 2 * cap == LANES and n * probe_count == LANES and span == 2 * LANES
        and power_of_two(clusters) and power_of_two(per_device) and power_of_two(probe_count)
        and clusters <= LANES and per_device == cap
        and clusters * per_device * n * cap < 2**23 and width % LANES == 0 and held < 32 * 2**20
    )
    chosen = fused_body if fits else routed_body
    return chosen(queries, probes, passages, centroids, counts)


def solution(mesh):
    in_specs = (
        P(("groups", "owner"), None),
        P(("groups", "owner"), None),
        P("owner", None, None),
        P("owner", None),
        P("owner"),
    )
    out_specs = (P(("groups", "owner"), None, None), P(("groups", "owner")))
    return jax.shard_map(body, mesh=mesh, in_specs=in_specs, out_specs=out_specs, check_vma=False)
```
